32 devices in a mesh: row: 8 (over z, y), col: 4 (over x, core).
Axes of the slice: x: 2, y: 2, z: 4, core: 2. Of those that a mesh axis runs over, the one named last changes fastest.
Arguments:
- weights: float32 [2, 4, 2048, 8, 1024], P(None, None, 'row', None, 'col'), may hold values from -6 to 6
Outputs:
- trailing: float32 [2, 4, 2048, 8, 1024], P(None, None, 'row', None, 'col')
- diagonal: float32 [2, 12], replicated
- superdiag: float32 [2, 12], replicated
The draws below stay inside these ranges and needn't reach their ends.
All inputs are finite; a program needn't handle non-finite values.
Results may differ from the reference program's by a relative error of at most 0.0003.
Values sent between devices are 32-bit elements; how exact they have to be, the bound alone decides.
A program may use at most 128 MiB of HBM per device.

```python
import jax
import jax.numpy as jnp
from jax import lax

N = 8192
TILE = 256
STEPS = 6
PANELS = 2
MATS = 2
RCYC = 4
CCYC = 8
N_ROW = 8
N_COL = 4


def level_of(rng, shape, split, low, top_value):
    loudness = 1.0
    for position, shards_of in split:
        draws = jax.random.uniform(jax.random.fold_in(jax.random.fold_in(rng, 6), position), (shards_of,), jnp.float32, low / len(split), top_value / len(split))
        loudness = loudness * jnp.repeat(jnp.exp(draws), shape[position] // shards_of).reshape((-1,) + (1,) * (len(shape) - 1 - position))
    return loudness


def scatter_about(own_key, dims, width, limit, pieces=(), kind=jnp.bfloat16):
    values = jax.random.normal(own_key, dims, jnp.float32) * width
    if len(pieces) > 0:
        values = level_of(own_key, dims, pieces, -0.22, 0.18) * values
    return jnp.clip(values, min=-limit, max=limit).astype(kind)


def setup_inputs(seed: int = 0) -> dict:
    key_list = jax.random.split(jax.random.key(seed), 2)
    return {
        "weights": scatter_about(key_list[0], (MATS, RCYC, N_ROW * TILE, CCYC, N_COL * TILE), 1.0, 6.0, ((2, 8), (4, 4)), jnp.float32),
    }


def contract(form, left, right):
    return jnp.einsum(form, left, right, precision=lax.Precision.HIGHEST)

def reflect(leading, squares):
    length = jnp.sqrt(squares)
    divisor = jnp.maximum(leading + length, 1.0)
    factor = (leading + length) / jnp.maximum(length, 1.0)
    return (divisor, factor, -length)

def reference(weights):
    mats = weights.reshape(MATS, N, N)
    global_ids = jnp.arange(N, dtype=jnp.int32)
    diag_list = []
    super_list = []
    for panel_at in range(PANELS):
        first_at = panel_at * STEPS
        col_refl = jnp.zeros((MATS, STEPS, N), jnp.float32)
        col_aux = jnp.zeros((MATS, STEPS, N), jnp.float32)
        row_aux = jnp.zeros((MATS, STEPS, N), jnp.float32)
        row_refl = jnp.zeros((MATS, STEPS, N), jnp.float32)
        for step_at in range(STEPS):
            pivot = first_at + step_at
            col_piece = mats[:, :, pivot] - contract('mp,mpr->mr', row_aux[:, :, pivot], col_refl) - contract('mp,mpr->mr', row_refl[:, :, pivot], col_aux)
            col_piece = jnp.where(global_ids >= pivot, col_piece, 0.0)
            divisor, factor, bidiag = reflect(col_piece[:, pivot], lax.optimization_barrier(jnp.sum(col_piece * col_piece, axis=1)))
            col_vec = jnp.where(global_ids == pivot, 1.0, col_piece / divisor[:, None])
            col_refl = col_refl.at[:, step_at].set(col_vec)
            weighs_one = contract('mpr,mr->mp', col_refl, col_vec)
            weighs_two = contract('mpr,mr->mp', col_aux, col_vec)
            col_img = factor[:, None] * (contract('mrc,mr->mc', mats, col_vec) - contract('mp,mpc->mc', weighs_one, row_aux) - contract('mp,mpc->mc', weighs_two, row_refl))
            col_img = jnp.where(global_ids > pivot, col_img, 0.0)
            row_aux = row_aux.at[:, step_at].set(col_img)
            row_piece = mats[:, pivot, :] - contract('mp,mpc->mc', col_refl[:, :, pivot], row_aux) - contract('mp,mpc->mc', col_aux[:, :, pivot], row_refl)
            row_piece = jnp.where(global_ids > pivot, row_piece, 0.0)
            divisor2, factor2, bidiag2 = reflect(row_piece[:, pivot + 1], lax.optimization_barrier(jnp.sum(row_piece * row_piece, axis=1)))
            row_vec = jnp.where(global_ids == pivot + 1, 1.0, row_piece / divisor2[:, None])
            row_refl = row_refl.at[:, step_at].set(row_vec)
            dots_one = contract('mpc,mc->mp', row_aux, row_vec)
            dots_two = contract('mpc,mc->mp', row_refl, row_vec)
            row_img = factor2[:, None] * (contract('mrc,mc->mr', mats, row_vec) - contract('mp,mpr->mr', dots_one, col_refl) - contract('mp,mpr->mr', dots_two, col_aux))
            row_img = jnp.where(global_ids > pivot, row_img, 0.0)
            col_aux = col_aux.at[:, step_at].set(row_img)
            diag_list.append(bidiag)
            super_list.append(bidiag2)
        mats = mats - contract('mpr,mpc->mrc', col_refl, row_aux) - contract('mpr,mpc->mrc', col_aux, row_refl)
    done = PANELS * STEPS
    inside = (global_ids[:, None] >= done) & (global_ids[None, :] >= done)
    trailing = jnp.where(inside[None], mats, 0.0).reshape(weights.shape)
    return (trailing, jnp.stack(diag_list, axis=1), jnp.stack(super_list, axis=1))
```

```python
import functools

import jax
import jax.numpy as jnp
from jax import lax
from jax.experimental import pallas as pl
from jax.experimental.pallas import tpu as pltpu
from jax.sharding import PartitionSpec as P

STEPS = 6
PANELS = 2
TOTAL = STEPS * PANELS
SLOTS = 2 * TOTAL
LANES = 128
SUB = 8
ROWS_KEPT = 16
SUPER_AT = 64
MESH = pl.DeviceIdType.MESH
F32 = jnp.float32


def reflect(leading, squares):
    length = jnp.sqrt(squares)
    divisor = jnp.maximum(leading + length, 1.0)
    factor = (leading + length) / jnp.maximum(length, 1.0)
    return (divisor, factor, -length)


def partner(me, d, count):
    if count & (count - 1):
        return lax.rem(me + d, count), lax.rem(me - d + count, count)
    to = me
    bit = 1
    while bit < count:
        if d & bit:
            to = to + bit - 2 * bit * lax.rem(me // bit, 2)
        bit *= 2
    return to, to


def peers(axis, count):
    me = lax.axis_index(axis)
    return [partner(me, d, count) for d in range(count - 1, 0, -1)]


def row_ids(blocks, tile_len, devices, place):
    at = lax.broadcasted_iota(jnp.int32, (blocks, LANES), 0) * LANES
    at = at + lax.broadcasted_iota(jnp.int32, (blocks, LANES), 1)
    return at // tile_len * (devices * tile_len) + place * tile_len + at % tile_len


def col_ids(pieces, tile_len, devices, place):
    cycles = pieces * LANES // tile_len
    q = lax.broadcasted_iota(jnp.int32, (pieces, LANES), 0)
    lane = lax.broadcasted_iota(jnp.int32, (pieces, LANES), 1)
    return q % cycles * (devices * tile_len) + place * tile_len + q // cycles * LANES + lane


def tree(parts):
    while len(parts) > 1:
        parts = [
            parts[i] + parts[i + 1] if i + 1 < len(parts) else parts[i]
            for i in range(0, len(parts), 2)
        ]
    return parts[0]


def put_row(ref, m, at, dense):
    span = pl.ds(pl.multiple_of(at // SUB * SUB, SUB), SUB)
    here = lax.broadcasted_iota(jnp.int32, (SUB, LANES), 0) == lax.rem(at, SUB)
    for q in range(dense.shape[0]):
        cut = slice(q * LANES, (q + 1) * LANES)
        ref[m, span, cut] = jnp.where(here, dense[q : q + 1], ref[m, span, cut])


def small_row(dots, picks, squares, leading):
    at = lax.broadcasted_iota(jnp.int32, (SUB, LANES), 0)
    extra = jnp.where(at == 0, squares, jnp.where(at == 1, leading, 0.0))
    rest = jnp.zeros((LANES - 2 * SLOTS - SUB, LANES), F32)
    tile = jnp.concatenate([dots, picks, extra, rest], axis=0)
    return jnp.sum(tile.T, axis=0, keepdims=True)


def kernel(
    row_n, col_n, tile_len, w, mats, vx, yu, bid,
    cols, rows, cd, rd, base_c, base_r, row_big, row_small, col_big, col_small,
    load_sem, rows_sem, row_send, row_recv, col_send, col_recv,
    first_send, first_recv, cols_send, cols_recv, rows_send, rows_recv,
):
    batch_n, height, pieces, _ = w.shape
    blocks = height // LANES
    row_place = lax.axis_index("row")
    col_place = lax.axis_index("col")
    row_peers = peers("row", row_n)
    col_peers = peers("col", col_n)

    def load(m, q):
        return pltpu.make_async_copy(
            w.at[m, :, q, :], mats.at[m, :, q * LANES : (q + 1) * LANES], load_sem.at[m, q]
        )

    def load_rows(m):
        return pltpu.make_async_copy(w.at[m, pl.ds(0, ROWS_KEPT)], rows.at[m], rows_sem.at[m])

    for m in range(batch_n):
        load(m, 0).start()

    @pl.when(row_place == 0)
    def _():
        for m in range(batch_n):
            load_rows(m).start()

    for m in range(batch_n):
        for q in range(1, pieces):
            load(m, q).start()

    vx[...] = jnp.zeros_like(vx)
    yu[...] = jnp.zeros_like(yu)
    bid[...] = jnp.zeros_like(bid)
    rd[...] = jnp.zeros_like(rd)
    col_big[...] = jnp.zeros_like(col_big)
    col_small[...] = jnp.zeros_like(col_small)

    barrier = pltpu.get_barrier_semaphore()
    for axis, count, others in (("row", row_n, row_peers), ("col", col_n, col_peers)):
        for to, _ in others:
            pl.semaphore_signal(barrier, inc=1, device_id={axis: to}, device_id_type=MESH)
    pl.semaphore_wait(barrier, row_n + col_n - 2)

    def remote(ref, send, recv, axis, to):
        return pltpu.make_async_remote_copy(
            src_ref=ref,
            dst_ref=ref,
            send_sem=send,
            recv_sem=recv,
            device_id={axis: to},
            device_id_type=MESH,
        )

    def first_col(at, to):
        return remote(cols.at[:, 0], first_send.at[at], first_recv, "col", to)

    def later_cols(at, to):
        return remote(
            cols.at[:, pl.ds(1, TOTAL)], cols_send.at[at], cols_recv, "col", to
        )

    def row_copy(m, k, at, to):
        return remote(rows.at[m, k], rows_send.at[m, at], rows_recv.at[m, k], "row", to)

    for m in range(batch_n):
        load(m, 0).wait()

    @pl.when(col_place == 0)
    def _():
        for m in range(batch_n):
            for b in range(blocks):
                turned = mats[m, b * LANES : (b + 1) * LANES, 0:LANES].T
                for j in range(TOTAL + 1):
                    cols[m, j, b : b + 1, :] = turned[j : j + 1]
        for at, (to, _) in enumerate(col_peers):
            first_col(at, to).start()
        for at, (to, _) in enumerate(col_peers):
            later_cols(at, to).start()

    @pl.when(row_place == 0)
    def _():
        for m in range(batch_n):
            load_rows(m).wait()
            for at, (to, _) in enumerate(row_peers):
                row_copy(m, 0, at, to).start()

    @pl.when(col_place != 0)
    def _():
        first_col(0, 0).wait_recv()

    grow = row_ids(blocks, tile_len, row_n, row_place)
    gcol = col_ids(pieces, tile_len, col_n, col_place)
    lane = lax.broadcasted_iota(jnp.int32, (1, LANES), 1)
    own_row = jnp.where(row_place == 0, lane, -1)
    own_col = jnp.where(col_place == 0, lane, -1)
    row_at = lax.broadcasted_iota(jnp.int32, (SUB, LANES), 0)
    lane_at = lax.broadcasted_iota(jnp.int32, (SUB, LANES), 1)

    def exchange(axis, others, par, m, which, ref, sems):
        me = lax.axis_index(axis)
        send, recv = sems
        span = pl.ds(me, 1) if which == 0 else me
        sends = [
            remote(ref.at[par, m, span], send.at[m, which, at], recv.at[par, m, which, me], axis, to)
            for at, (to, _) in enumerate(others)
        ]
        return sends

    def arrivals(axis, others, par, m, which, ref, sems):
        send, recv = sems
        return [
            remote(
                ref.at[par, m, pl.ds(source, 1) if which == 0 else source],
                send.at[m, which, at],
                recv.at[par, m, which, source],
                axis,
                source,
            )
            for at, (_, source) in enumerate(others)
        ]

    row_args = ("row", row_peers)
    col_args = ("col", col_peers)
    row_sems = (row_send, row_recv)
    col_sems = (col_send, col_recv)

    def take(args, par, m, which, ref, sems):
        for copy in arrivals(*args, par, m, which, ref, sems):
            copy.wait_recv()
        for copy in exchange(*args, par, m, which, ref, sems):
            copy.wait_send()

    def sums_of(ref, par, m):
        total = jnp.sum(ref[par, m], axis=0, keepdims=True)
        turned = jnp.broadcast_to(total, (LANES, LANES)).T
        dots = turned[0:SLOTS]
        picks = turned[SLOTS : 2 * SLOTS]
        squares = turned[2 * SLOTS : 2 * SLOTS + 1]
        leading = turned[2 * SLOTS + 1 : 2 * SLOTS + 2]
        divisor, factor, bidiag = reflect(leading, squares)
        remain = 1.0 - leading / divisor
        weight = dots / divisor + picks * remain
        return divisor, factor, bidiag, remain, weight, picks

    def before_col(k, m):
        par = lax.rem(k + 1, 2)

        @pl.when(k > 0)
        def _():
            take(col_args, par, m, 0, col_small, col_sems)

        divisor, factor, bidiag, remain, weight, picks = sums_of(col_small, par, m)
        bid[...] = jnp.where((row_at == m) & (lane_at == SUPER_AT - 1 + k), bidiag, bid[...])
        row_vec = jnp.where(gcol == k, 1.0, rd[m] / divisor)
        row_vec = jnp.where(k > 0, row_vec, 0.0)
        at = jnp.where(k > 0, TOTAL - 1 + k, 0)
        put_row(yu, m, at, row_vec)
        column = cols[m, k]
        for b in range(blocks):
            old = vx[m, :, b * LANES : (b + 1) * LANES]
            base_c[m, 0, b : b + 1, :] = factor * (
                column[b : b + 1] * remain - jnp.sum(weight * old, axis=0, keepdims=True)
            )
            base_c[m, 1, b : b + 1, :] = column[b : b + 1] - jnp.sum(
                picks * old, axis=0, keepdims=True
            )
        base_c[m, 2] = jnp.broadcast_to(factor / divisor, (blocks, LANES))

    def new_col(k, m):
        par = lax.rem(k + 1, 2)

        @pl.when(k > 0)
        def _():
            take(col_args, par, m, 1, col_big, col_sems)

        applied = tree([col_big[par, m, s] for s in range(col_n)])
        image = jnp.where(grow >= k, base_c[m, 2] * applied + base_c[m, 0], 0.0)
        at = jnp.where(k > 0, TOTAL - 1 + k, 0)
        put_row(vx, m, at, image)
        return image

    def col_half(k, m):
        par = lax.rem(k, 2)
        image = new_col(k, m)
        piece = jnp.where(grow >= k, base_c[m, 1] - image, 0.0)
        cd[m] = piece
        dots = tree(
            [
                vx[m, :, b * LANES : (b + 1) * LANES] * piece[b : b + 1]
                for b in range(blocks)
            ]
        )
        picks = jnp.where(own_row == k, vx[m, :, 0:LANES], 0.0)
        squares = jnp.sum(piece * piece, axis=0, keepdims=True)
        leading = jnp.sum(jnp.where(grow == k, piece, 0.0), axis=0, keepdims=True)
        small = small_row(dots, picks, squares, leading)
        total = [None] * pieces
        for b in range(blocks):
            scale = jnp.broadcast_to(cd[m, b : b + 1, :], (LANES, LANES)).T
            for g in range(LANES // SUB):
                span = pl.ds(b * LANES + g * SUB, SUB)
                by = scale[g * SUB : (g + 1) * SUB]
                for q in range(pieces):
                    part = mats[m, span, q * LANES : (q + 1) * LANES] * by
                    total[q] = part if total[q] is None else total[q] + part
            if b == blocks // 2 - 1:
                row_small[par, m, pl.ds(row_place, 1), :] = small
                for copy in exchange(*row_args, par, m, 0, row_small, row_sems):
                    copy.start()
        for q in range(pieces):
            row_big[par, m, row_place, q : q + 1, :] = jnp.sum(total[q], axis=0, keepdims=True)
        for copy in exchange(*row_args, par, m, 1, row_big, row_sems):
            copy.start()

        @pl.when((row_place == 0) & (k < TOTAL - 1))
        def _():
            for at, (to, _) in enumerate(row_peers):
                row_copy(m, k, at, to).wait_send()
            for at, (to, _) in enumerate(row_peers):
                row_copy(m, k + 1, at, to).start()

    def before_row(k, m):
        par = lax.rem(k, 2)
        take(row_args, par, m, 0, row_small, row_sems)

        @pl.when(row_place != 0)
        def _():
            row_copy(m, k, 0, 0).wait_recv()

        divisor, factor, bidiag, remain, weight, picks = sums_of(row_small, par, m)
        bid[...] = jnp.where((row_at == m) & (lane_at == k), bidiag, bid[...])
        col_vec = jnp.where(grow == k, 1.0, cd[m] / divisor)
        put_row(vx, m, k, col_vec)
        row = rows[m, k]
        for q in range(pieces):
            old = yu[m, :, q * LANES : (q + 1) * LANES]
            base_r[m, 0, q : q + 1, :] = factor * (
                row[q : q + 1] * remain - jnp.sum(weight * old, axis=0, keepdims=True)
            )
            base_r[m, 1, q : q + 1, :] = row[q : q + 1] - jnp.sum(
                picks * old, axis=0, keepdims=True
            )
        base_r[m, 2] = jnp.broadcast_to(factor / divisor, (pieces, LANES))

    def row_half(k, m):
        par = lax.rem(k, 2)
        take(row_args, par, m, 1, row_big, row_sems)
        trans = tree([row_big[par, m, s] for s in range(row_n)])
        image = jnp.where(gcol > k, base_r[m, 2] * trans + base_r[m, 0], 0.0)
        put_row(yu, m, k, image)
        piece = jnp.where(gcol > k, base_r[m, 1] - image, 0.0)
        rd[m] = piece
        dots = tree(
            [
                yu[m, :, q * LANES : (q + 1) * LANES] * piece[q : q + 1]
                for q in range(pieces)
            ]
        )
        picks = jnp.where(own_col == k + 1, yu[m, :, 0:LANES], 0.0)
        squares = jnp.sum(piece * piece, axis=0, keepdims=True)
        leading = jnp.sum(jnp.where(gcol == k + 1, piece, 0.0), axis=0, keepdims=True)
        small = small_row(dots, picks, squares, leading)
        scale = [
            jnp.broadcast_to(rd[m, q : q + 1, :], (SUB, LANES)) for q in range(pieces)
        ]
        for b in range(blocks):
            groups = []
            for g in range(LANES // SUB):
                span = pl.ds(b * LANES + g * SUB, SUB)
                groups.append(
                    tree(
                        [
                            mats[m, span, q * LANES : (q + 1) * LANES] * scale[q]
                            for q in range(pieces)
                        ]
                    )
                )
            turned = jnp.concatenate(groups, axis=0).T
            col_big[par, m, col_place, b : b + 1, :] = jnp.sum(turned, axis=0, keepdims=True)
            if b == blocks // 2 - 1:
                col_small[par, m, pl.ds(col_place, 1), :] = small
                for copy in exchange(*col_args, par, m, 0, col_small, col_sems):
                    copy.start()
        for copy in exchange(*col_args, par, m, 1, col_big, col_sems):
            copy.start()

    def step_body(k, carry):
        for m in range(batch_n):

            @pl.when(k == 0)
            def _():
                for q in range(1, pieces):
                    load(m, q).wait()

            before_col(k, m)
            col_half(k, m)
        for m in range(batch_n):
            before_row(k, m)
            row_half(k, m)

        @pl.when((k == 0) & (col_place != 0))
        def _():
            later_cols(0, 0).wait_recv()

        return carry

    lax.fori_loop(0, TOTAL, step_body, 0)
    for m in range(batch_n):
        before_col(TOTAL, m)
        new_col(TOTAL, m)

    @pl.when(col_place == 0)
    def _():
        for at, (to, _) in enumerate(col_peers):
            first_col(at, to).wait_send()
            later_cols(at, to).wait_send()

    @pl.when(row_place == 0)
    def _():
        for m in range(batch_n):
            for at, (to, _) in enumerate(row_peers):
                row_copy(m, TOTAL - 1, at, to).wait_send()


def factor_all(w, row_n, col_n, tile_len):
    batch_n, height, pieces, _ = w.shape
    width = pieces * LANES
    blocks = height // LANES
    whole = pl.BlockSpec(memory_space=pltpu.VMEM)
    return pl.pallas_call(
        functools.partial(kernel, row_n, col_n, tile_len),
        out_shape=(
            jax.ShapeDtypeStruct((batch_n, height, width), F32),
            jax.ShapeDtypeStruct((batch_n, SLOTS, height), F32),
            jax.ShapeDtypeStruct((batch_n, SLOTS, width), F32),
            jax.ShapeDtypeStruct((SUB, LANES), F32),
        ),
        in_specs=[pl.BlockSpec(memory_space=pltpu.HBM)],
        out_specs=(whole, whole, whole, whole),
        scratch_shapes=[
            pltpu.VMEM((batch_n, TOTAL + 1, blocks, LANES), F32),
            pltpu.VMEM((batch_n, ROWS_KEPT, pieces, LANES), F32),
            pltpu.VMEM((batch_n, blocks, LANES), F32),
            pltpu.VMEM((batch_n, pieces, LANES), F32),
            pltpu.VMEM((batch_n, 3, blocks, LANES), F32),
            pltpu.VMEM((batch_n, 3, pieces, LANES), F32),
            pltpu.VMEM((2, batch_n, row_n, pieces, LANES), F32),
            pltpu.VMEM((2, batch_n, row_n, LANES), F32),
            pltpu.VMEM((2, batch_n, col_n, blocks, LANES), F32),
            pltpu.VMEM((2, batch_n, col_n, LANES), F32),
            pltpu.SemaphoreType.DMA((batch_n, pieces)),
            pltpu.SemaphoreType.DMA((batch_n,)),
            pltpu.SemaphoreType.DMA((batch_n, 2, row_n)),
            pltpu.SemaphoreType.DMA((2, batch_n, 2, row_n)),
            pltpu.SemaphoreType.DMA((batch_n, 2, col_n)),
            pltpu.SemaphoreType.DMA((2, batch_n, 2, col_n)),
            pltpu.SemaphoreType.DMA((col_n,)),
            pltpu.SemaphoreType.DMA,
            pltpu.SemaphoreType.DMA((col_n,)),
            pltpu.SemaphoreType.DMA,
            pltpu.SemaphoreType.DMA((batch_n, row_n)),
            pltpu.SemaphoreType.DMA((batch_n, TOTAL)),
        ],
        compiler_params=pltpu.CompilerParams(
            collective_id=0, has_side_effects=True, vmem_limit_bytes=24 * 1024 * 1024
        ),
    )(w)


def update_kernel(row_n, col_n, tile_len, mats, vx, yu, out, left, right, stage, sems):
    batch_n, height, width = mats.shape
    pieces = width // LANES
    blocks = height // LANES
    row_place = lax.axis_index("row")
    col_place = lax.axis_index("col")
    slots = stage.shape[0]
    empty = jnp.zeros((LANES - 4 * SLOTS, LANES), F32)

    def halves(value):
        high = value.astype(jnp.bfloat16).astype(F32)
        return high, value - high

    for m in range(batch_n):
        for b in range(blocks):
            high, low = halves(vx[m, :, b * LANES : (b + 1) * LANES])
            stack = jnp.concatenate([high, high, low, low, empty], axis=0)
            left[m, b * LANES : (b + 1) * LANES, :] = stack.T.astype(jnp.bfloat16)
        for q in range(pieces):
            high, low = halves(yu[m, :, q * LANES : (q + 1) * LANES])
            stack = jnp.concatenate([high, low, high, low, empty], axis=0)
            right[m, :, q * LANES : (q + 1) * LANES] = stack.astype(jnp.bfloat16)

    def copies(at):
        slot = lax.rem(at, slots)
        m = at // blocks
        span = pl.ds(pl.multiple_of(lax.rem(at, blocks) * LANES, LANES), LANES)
        return [
            pltpu.make_async_copy(
                stage.at[slot, :, q * LANES : (q + 1) * LANES],
                out.at[m, span, q, :],
                sems.at[slot, q],
            )
            for q in range(pieces)
        ]

    row_at = lax.broadcasted_iota(jnp.int32, (LANES, LANES), 0)
    lane_at = lax.broadcasted_iota(jnp.int32, (LANES, LANES), 1)

    @pl.loop(0, batch_n * blocks)
    def _(at):
        slot = lax.rem(at, slots)
        m = at // blocks
        block = lax.rem(at, blocks)
        span = pl.ds(pl.multiple_of(block * LANES, LANES), LANES)

        @pl.when(at >= slots)
        def _():
            for copy in copies(at - slots):
                copy.wait()

        for q in range(0, pieces, 2):
            cut = slice(q * LANES, (q + 2) * LANES)
            change = jnp.dot(left[m, span, :], right[m, :, cut], preferred_element_type=F32)
            stage[slot, :, cut] = mats[m, span, cut] - change

        @pl.when(col_place == 0)
        def _():
            stage[slot, :, 0:LANES] = jnp.where(lane_at < TOTAL, 0.0, stage[slot, :, 0:LANES])

        @pl.when((row_place == 0) & (block == 0))
        def _():
            stage[slot, 0:ROWS_KEPT, :] = jnp.where(
                lax.broadcasted_iota(jnp.int32, (ROWS_KEPT, width), 0) < TOTAL,
                0.0,
                stage[slot, 0:ROWS_KEPT, :],
            )

        for copy in copies(at):
            copy.start()

    for at in range(batch_n * blocks - slots, batch_n * blocks):
        for copy in copies(at):
            copy.wait()


def update_all(mats, vx, yu, row_n, col_n, tile_len):
    batch_n, height, width = mats.shape
    pieces = width // LANES
    whole = pl.BlockSpec(memory_space=pltpu.VMEM)
    slots = 4
    return pl.pallas_call(
        functools.partial(update_kernel, row_n, col_n, tile_len),
        out_shape=jax.ShapeDtypeStruct((batch_n, height, pieces, LANES), F32),
        in_specs=[whole, whole, whole],
        out_specs=pl.BlockSpec(memory_space=pltpu.HBM),
        scratch_shapes=[
            pltpu.VMEM((batch_n, height, LANES), jnp.bfloat16),
            pltpu.VMEM((batch_n, LANES, width), jnp.bfloat16),
            pltpu.VMEM((slots, LANES, width), F32),
            pltpu.SemaphoreType.DMA((slots, pieces)),
        ],
        compiler_params=pltpu.CompilerParams(vmem_limit_bytes=24 * 1024 * 1024),
    )(mats, vx, yu)


def per_device(weights):
    batch_n, row_cycles, tile_len, col_cycles, _ = weights.shape
    height = row_cycles * tile_len
    parts = tile_len // LANES
    row_n = lax.axis_size("row")
    col_n = lax.axis_size("col")
    w = weights.reshape(batch_n, row_cycles, tile_len, col_cycles, parts, LANES)
    w = w.transpose(0, 1, 2, 4, 3, 5).reshape(batch_n, height, parts * col_cycles, LANES)
    mats, vx, yu, bid = factor_all(w, row_n, col_n, tile_len)
    out = update_all(mats, vx, yu, row_n, col_n, tile_len)
    out = out.reshape(batch_n, row_cycles, tile_len, parts, col_cycles, LANES)
    trailing = out.transpose(0, 1, 2, 4, 3, 5).reshape(weights.shape)
    return (trailing, bid[:batch_n, :TOTAL], bid[:batch_n, SUPER_AT : SUPER_AT + TOTAL])


def solution(mesh):
    placed = (P(None, None, "row", None, "col"),)
    return jax.shard_map(
        per_device,
        mesh=mesh,
        in_specs=placed,
        out_specs=(P(None, None, "row", None, "col"), P(), P()),
        check_vma=False,
    )
```

```python
import functools

import jax
import jax.numpy as jnp
from jax import lax
from jax.experimental import pallas as pl
from jax.experimental.pallas import tpu as pltpu
from jax.sharding import PartitionSpec as P

STEPS = 6
PANELS = 2
TOTAL = STEPS * PANELS
SLOTS = 2 * TOTAL
LANES = 128
SUB = 8
ROWS_KEPT = 16
MESH = pl.DeviceIdType.MESH
F32 = jnp.float32


def reflect(leading, squares):
    length = jnp.sqrt(squares)
    divisor = jnp.maximum(leading + length, 1.0)
    factor = (leading + length) / jnp.maximum(length, 1.0)
    return (divisor, factor, -length)


def partner(me, d, count):
    if count & (count - 1):
        return lax.rem(me + d, count), lax.rem(me - d + count, count)
    to = me
    bit = 1
    while bit < count:
        if d & bit:
            to = to + bit - 2 * bit * lax.rem(me // bit, 2)
        bit *= 2
    return to, to


def peers(axis, count):
    me = lax.axis_index(axis)
    return [partner(me, d, count) for d in range(count - 1, 0, -1)]


def row_ids(blocks, tile_len, devices, place):
    at = lax.broadcasted_iota(jnp.int32, (blocks, LANES), 0) * LANES
    at = at + lax.broadcasted_iota(jnp.int32, (blocks, LANES), 1)
    return at // tile_len * (devices * tile_len) + place * tile_len + at % tile_len


def col_ids(pieces, tile_len, devices, place):
    cycles = pieces * LANES // tile_len
    q = lax.broadcasted_iota(jnp.int32, (pieces, LANES), 0)
    lane = lax.broadcasted_iota(jnp.int32, (pieces, LANES), 1)
    return q % cycles * (devices * tile_len) + place * tile_len + q // cycles * LANES + lane


def tree(parts):
    while len(parts) > 1:
        parts = [
            parts[i] + parts[i + 1] if i + 1 < len(parts) else parts[i]
            for i in range(0, len(parts), 2)
        ]
    return parts[0]


def put_row(ref, m, at, dense):
    span = pl.ds(pl.multiple_of(at // SUB * SUB, SUB), SUB)
    here = lax.broadcasted_iota(jnp.int32, (SUB, LANES), 0) == lax.rem(at, SUB)
    for q in range(dense.shape[0]):
        cut = slice(q * LANES, (q + 1) * LANES)
        ref[m, span, cut] = jnp.where(here, dense[q : q + 1], ref[m, span, cut])


def small_row(dots, picks, squares, leading):
    at = lax.broadcasted_iota(jnp.int32, (SUB, LANES), 0)
    extra = jnp.where(at == 0, squares, jnp.where(at == 1, leading, 0.0))
    rest = jnp.zeros((LANES - 2 * SLOTS - SUB, LANES), F32)
    tile = jnp.concatenate([dots, picks, extra, rest], axis=0)
    return jnp.sum(tile.T, axis=0, keepdims=True)


def kernel(
    row_n, col_n, tile_len, w, mats, vx, yu, bid,
    cols, rows, spread, cd, rd, base_c, base_r, row_big, row_small, col_big, col_small,
    load_sem, rows_sem, row_send, row_recv, col_send, col_recv,
    first_send, first_recv, cols_send, cols_recv, rows_send, rows_recv,
):
    batch_n, height, pieces, _ = w.shape
    blocks = height // LANES
    row_place = lax.axis_index("row")
    col_place = lax.axis_index("col")
    row_peers = peers("row", row_n)
    col_peers = peers("col", col_n)

    def load(m, q):
        return pltpu.make_async_copy(
            w.at[m, :, q, :], mats.at[m, :, q * LANES : (q + 1) * LANES], load_sem.at[m, q]
        )

    def load_rows(m):
        return pltpu.make_async_copy(w.at[m, pl.ds(0, ROWS_KEPT)], rows.at[m], rows_sem.at[m])

    for m in range(batch_n):
        load(m, 0).start()

    @pl.when(row_place == 0)
    def _():
        for m in range(batch_n):
            load_rows(m).start()

    for m in range(batch_n):
        for q in range(1, pieces):
            load(m, q).start()

    vx[...] = jnp.zeros_like(vx)
    yu[...] = jnp.zeros_like(yu)
    bid[...] = jnp.zeros_like(bid)
    rd[...] = jnp.zeros_like(rd)
    col_big[...] = jnp.zeros_like(col_big)
    col_small[...] = jnp.zeros_like(col_small)

    barrier = pltpu.get_barrier_semaphore()
    for axis, count, others in (("row", row_n, row_peers), ("col", col_n, col_peers)):
        for to, _ in others:
            pl.semaphore_signal(barrier, inc=1, device_id={axis: to}, device_id_type=MESH)
    pl.semaphore_wait(barrier, row_n + col_n - 2)

    def remote(ref, send, recv, axis, to):
        return pltpu.make_async_remote_copy(
            src_ref=ref,
            dst_ref=ref,
            send_sem=send,
            recv_sem=recv,
            device_id={axis: to},
            device_id_type=MESH,
        )

    def first_col(at, to):
        return remote(cols.at[:, 0], first_send.at[at], first_recv, "col", to)

    def later_cols(at, to):
        return remote(
            cols.at[:, pl.ds(1, TOTAL)], cols_send.at[at], cols_recv, "col", to
        )

    def row_copy(m, k, at, to):
        return remote(rows.at[m, k], rows_send.at[m, at], rows_recv.at[m, k], "row", to)

    for m in range(batch_n):
        load(m, 0).wait()

    @pl.when(col_place == 0)
    def _():
        for m in range(batch_n):
            for b in range(blocks):
                turned = mats[m, b * LANES : (b + 1) * LANES, 0:LANES].T
                for j in range(TOTAL + 1):
                    cols[m, j, b : b + 1, :] = turned[j : j + 1]
        for at, (to, _) in enumerate(col_peers):
            first_col(at, to).start()
        for at, (to, _) in enumerate(col_peers):
            later_cols(at, to).start()

    @pl.when(row_place == 0)
    def _():
        for m in range(batch_n):
            load_rows(m).wait()
            for at, (to, _) in enumerate(row_peers):
                row_copy(m, 0, at, to).start()

    @pl.when(col_place != 0)
    def _():
        first_col(0, 0).wait_recv()

    grow = row_ids(blocks, tile_len, row_n, row_place)
    gcol = col_ids(pieces, tile_len, col_n, col_place)
    lane = lax.broadcasted_iota(jnp.int32, (1, LANES), 1)
    own_row = jnp.where(row_place == 0, lane, -1)
    own_col = jnp.where(col_place == 0, lane, -1)
    row_at = lax.broadcasted_iota(jnp.int32, (SUB, LANES), 0)
    lane_at = lax.broadcasted_iota(jnp.int32, (SUB, LANES), 1)

    def post(axis, others, par, m, which, ref, sems):
        me = lax.axis_index(axis)
        send, recv = sems
        span = pl.ds(me, 1) if which == 0 else me
        for to, _ in others:
            remote(
                ref.at[par, m, span], send.at[m, which], recv.at[par, m, which], axis, to
            ).start()

    def all_of(axis, others, par, m, which, ref, sems):
        send, recv = sems
        return remote(
            ref.at[par, m, pl.ds(0, len(others))],
            send.at[m, which],
            recv.at[par, m, which],
            axis,
            others[0][0],
        )

    row_args = ("row", row_peers)
    col_args = ("col", col_peers)
    row_sems = (row_send, row_recv)
    col_sems = (col_send, col_recv)

    def take(args, par, m, which, ref, sems):
        all_of(*args, par, m, which, ref, sems).wait_recv()

    def sent(args, par, m, ref_small, ref_big, sems):
        all_of(*args, par, m, 0, ref_small, sems).wait_send()
        all_of(*args, par, m, 1, ref_big, sems).wait_send()

    def sums_of(ref, par, m):
        total = jnp.sum(ref[par, m], axis=0, keepdims=True)
        turned = jnp.broadcast_to(total, (LANES, LANES)).T
        dots = turned[0:SLOTS]
        picks = turned[SLOTS : 2 * SLOTS]
        squares = turned[2 * SLOTS : 2 * SLOTS + 1]
        leading = turned[2 * SLOTS + 1 : 2 * SLOTS + 2]
        divisor, factor, bidiag = reflect(leading, squares)
        remain = 1.0 - leading / divisor
        weight = dots / divisor + picks * remain
        return divisor, factor, bidiag, remain, weight, picks

    def before_col(k, m):
        par = lax.rem(k + 1, 2)

        @pl.when(k > 0)
        def _():
            sent(row_args, par, m, row_small, row_big, row_sems)
            take(col_args, par, m, 0, col_small, col_sems)

        divisor, factor, bidiag, remain, weight, picks = sums_of(col_small, par, m)
        bid[1] = jnp.where((row_at == m) & (lane_at == k - 1), bidiag, bid[1])
        row_vec = jnp.where(gcol == k, 1.0, rd[m] / divisor)
        row_vec = jnp.where(k > 0, row_vec, 0.0)
        at = jnp.where(k > 0, TOTAL - 1 + k, 0)
        put_row(yu, m, at, row_vec)
        column = cols[m, k]
        for b in range(blocks):
            old = vx[m, :, b * LANES : (b + 1) * LANES]
            base_c[m, 0, b : b + 1, :] = factor * (
                column[b : b + 1] * remain - jnp.sum(weight * old, axis=0, keepdims=True)
            )
            base_c[m, 1, b : b + 1, :] = column[b : b + 1] - jnp.sum(
                picks * old, axis=0, keepdims=True
            )
        base_c[m, 2] = jnp.broadcast_to(factor / divisor, (blocks, LANES))

    def new_col(k, m):
        par = lax.rem(k + 1, 2)

        @pl.when(k > 0)
        def _():
            take(col_args, par, m, 1, col_big, col_sems)

        applied = tree([col_big[par, m, s] for s in range(col_n)])
        image = jnp.where(grow >= k, base_c[m, 2] * applied + base_c[m, 0], 0.0)
        at = jnp.where(k > 0, TOTAL - 1 + k, 0)
        put_row(vx, m, at, image)
        return image

    def col_half(k, m):
        par = lax.rem(k, 2)
        image = new_col(k, m)
        piece = jnp.where(grow >= k, base_c[m, 1] - image, 0.0)
        cd[m] = piece
        for b in range(blocks):
            spread[b * LANES : (b + 1) * LANES, :] = jnp.broadcast_to(
                cd[m, b : b + 1, :], (LANES, LANES)
            ).T
        dots = tree(
            [
                vx[m, :, b * LANES : (b + 1) * LANES] * piece[b : b + 1]
                for b in range(blocks)
            ]
        )
        picks = jnp.where(own_row == k, vx[m, :, 0:LANES], 0.0)
        squares = jnp.sum(piece * piece, axis=0, keepdims=True)
        leading = jnp.sum(jnp.where(grow == k, piece, 0.0), axis=0, keepdims=True)
        small = small_row(dots, picks, squares, leading)
        total = [None] * pieces
        for b in range(blocks):
            for g in range(LANES // SUB):
                span = pl.ds(b * LANES + g * SUB, SUB)
                by = spread[span, :]
                for q in range(pieces):
                    part = mats[m, span, q * LANES : (q + 1) * LANES] * by
                    total[q] = part if total[q] is None else total[q] + part
            if b == blocks // 2 - 1:
                row_small[par, m, pl.ds(row_place, 1), :] = small
                post(*row_args, par, m, 0, row_small, row_sems)
        for q in range(pieces):
            row_big[par, m, row_place, q : q + 1, :] = jnp.sum(total[q], axis=0, keepdims=True)
        post(*row_args, par, m, 1, row_big, row_sems)

        @pl.when((row_place == 0) & (k < TOTAL - 1))
        def _():
            for at, (to, _) in enumerate(row_peers):
                row_copy(m, k, at, to).wait_send()
            for at, (to, _) in enumerate(row_peers):
                row_copy(m, k + 1, at, to).start()

    def before_row(k, m):
        par = lax.rem(k, 2)
        @pl.when(k > 0)
        def _():
            sent(col_args, par, m, col_small, col_big, col_sems)

        take(row_args, par, m, 0, row_small, row_sems)

        @pl.when(row_place != 0)
        def _():
            row_copy(m, k, 0, 0).wait_recv()

        divisor, factor, bidiag, remain, weight, picks = sums_of(row_small, par, m)
        bid[0] = jnp.where((row_at == m) & (lane_at == k), bidiag, bid[0])
        col_vec = jnp.where(grow == k, 1.0, cd[m] / divisor)
        put_row(vx, m, k, col_vec)
        row = rows[m, k]
        for q in range(pieces):
            old = yu[m, :, q * LANES : (q + 1) * LANES]
            base_r[m, 0, q : q + 1, :] = factor * (
                row[q : q + 1] * remain - jnp.sum(weight * old, axis=0, keepdims=True)
            )
            base_r[m, 1, q : q + 1, :] = row[q : q + 1] - jnp.sum(
                picks * old, axis=0, keepdims=True
            )
        base_r[m, 2] = jnp.broadcast_to(factor / divisor, (pieces, LANES))

    def row_half(k, m):
        par = lax.rem(k, 2)
        take(row_args, par, m, 1, row_big, row_sems)
        trans = tree([row_big[par, m, s] for s in range(row_n)])
        image = jnp.where(gcol > k, base_r[m, 2] * trans + base_r[m, 0], 0.0)
        put_row(yu, m, k, image)
        piece = jnp.where(gcol > k, base_r[m, 1] - image, 0.0)
        rd[m] = piece
        dots = tree(
            [
                yu[m, :, q * LANES : (q + 1) * LANES] * piece[q : q + 1]
                for q in range(pieces)
            ]
        )
        picks = jnp.where(own_col == k + 1, yu[m, :, 0:LANES], 0.0)
        squares = jnp.sum(piece * piece, axis=0, keepdims=True)
        leading = jnp.sum(jnp.where(gcol == k + 1, piece, 0.0), axis=0, keepdims=True)
        small = small_row(dots, picks, squares, leading)
        scale = [
            jnp.broadcast_to(rd[m, q : q + 1, :], (SUB, LANES)) for q in range(pieces)
        ]
        for b in range(blocks):
            groups = []
            for g in range(LANES // SUB):
                span = pl.ds(b * LANES + g * SUB, SUB)
                groups.append(
                    tree(
                        [
                            mats[m, span, q * LANES : (q + 1) * LANES] * scale[q]
                            for q in range(pieces)
                        ]
                    )
                )
            turned = jnp.concatenate(groups, axis=0).T
            col_big[par, m, col_place, b : b + 1, :] = jnp.sum(turned, axis=0, keepdims=True)
            if b == blocks // 2 - 1:
                col_small[par, m, pl.ds(col_place, 1), :] = small
                post(*col_args, par, m, 0, col_small, col_sems)
        post(*col_args, par, m, 1, col_big, col_sems)

    def step_body(k, carry):
        for m in range(batch_n):

            @pl.when(k == 0)
            def _():
                for q in range(1, pieces):
                    load(m, q).wait()

            before_col(k, m)
            col_half(k, m)
        for m in range(batch_n):
            before_row(k, m)
            row_half(k, m)

        @pl.when((k == 0) & (col_place != 0))
        def _():
            later_cols(0, 0).wait_recv()

        return carry

    lax.fori_loop(0, TOTAL, step_body, 0)
    for m in range(batch_n):
        before_col(TOTAL, m)
        new_col(TOTAL, m)
        sent(col_args, (TOTAL + 1) % 2, m, col_small, col_big, col_sems)

    @pl.when(col_place == 0)
    def _():
        for at, (to, _) in enumerate(col_peers):
            first_col(at, to).wait_send()
            later_cols(at, to).wait_send()

    @pl.when(row_place == 0)
    def _():
        for m in range(batch_n):
            for at, (to, _) in enumerate(row_peers):
                row_copy(m, TOTAL - 1, at, to).wait_send()


def factor_all(w, row_n, col_n, tile_len):
    batch_n, height, pieces, _ = w.shape
    width = pieces * LANES
    blocks = height // LANES
    whole = pl.BlockSpec(memory_space=pltpu.VMEM)
    return pl.pallas_call(
        functools.partial(kernel, row_n, col_n, tile_len),
        out_shape=(
            jax.ShapeDtypeStruct((batch_n, height, width), F32),
            jax.ShapeDtypeStruct((batch_n, SLOTS, height), F32),
            jax.ShapeDtypeStruct((batch_n, SLOTS, width), F32),
            jax.ShapeDtypeStruct((2, SUB, LANES), F32),
        ),
        in_specs=[pl.BlockSpec(memory_space=pltpu.HBM)],
        out_specs=(whole, whole, whole, whole),
        scratch_shapes=[
            pltpu.VMEM((batch_n, TOTAL + 1, blocks, LANES), F32),
            pltpu.VMEM((batch_n, ROWS_KEPT, pieces, LANES), F32),
            pltpu.VMEM((height, LANES), F32),
            pltpu.VMEM((batch_n, blocks, LANES), F32),
            pltpu.VMEM((batch_n, pieces, LANES), F32),
            pltpu.VMEM((batch_n, 3, blocks, LANES), F32),
            pltpu.VMEM((batch_n, 3, pieces, LANES), F32),
            pltpu.VMEM((2, batch_n, row_n, pieces, LANES), F32),
            pltpu.VMEM((2, batch_n, row_n, LANES), F32),
            pltpu.VMEM((2, batch_n, col_n, blocks, LANES), F32),
            pltpu.VMEM((2, batch_n, col_n, LANES), F32),
            pltpu.SemaphoreType.DMA((batch_n, pieces)),
            pltpu.SemaphoreType.DMA((batch_n,)),
            pltpu.SemaphoreType.DMA((batch_n, 2)),
            pltpu.SemaphoreType.DMA((2, batch_n, 2)),
            pltpu.SemaphoreType.DMA((batch_n, 2)),
            pltpu.SemaphoreType.DMA((2, batch_n, 2)),
            pltpu.SemaphoreType.DMA((col_n,)),
            pltpu.SemaphoreType.DMA,
            pltpu.SemaphoreType.DMA((col_n,)),
            pltpu.SemaphoreType.DMA,
            pltpu.SemaphoreType.DMA((batch_n, row_n)),
            pltpu.SemaphoreType.DMA((batch_n, TOTAL)),
        ],
        compiler_params=pltpu.CompilerParams(
            collective_id=0, has_side_effects=True, vmem_limit_bytes=24 * 1024 * 1024
        ),
    )(w)


def update_kernel(mats, vx, yu, bid, out, diagonal, superdiag, left, right, stage, sems):
    batch_n, height, width = mats.shape
    pieces = width // LANES
    blocks = height // LANES
    row_place = lax.axis_index("row")
    col_place = lax.axis_index("col")
    slots = stage.shape[0]
    diagonal[...] = bid[0, 0:batch_n, 0:TOTAL]
    superdiag[...] = bid[1, 0:batch_n, 0:TOTAL]
    empty = jnp.zeros((LANES - 4 * SLOTS, LANES), F32)

    def halves(value):
        high = value.astype(jnp.bfloat16).astype(F32)
        return high, value - high

    for m in range(batch_n):
        for b in range(blocks):
            high, low = halves(vx[m, :, b * LANES : (b + 1) * LANES])
            stack = jnp.concatenate([high, high, low, low, empty], axis=0)
            left[m, b * LANES : (b + 1) * LANES, :] = stack.T.astype(jnp.bfloat16)
        for q in range(pieces):
            high, low = halves(yu[m, :, q * LANES : (q + 1) * LANES])
            stack = jnp.concatenate([high, low, high, low, empty], axis=0)
            right[m, :, q * LANES : (q + 1) * LANES] = stack.astype(jnp.bfloat16)

    def copies(at):
        slot = lax.rem(at, slots)
        m = at // blocks
        span = pl.ds(pl.multiple_of(lax.rem(at, blocks) * LANES, LANES), LANES)
        return [
            pltpu.make_async_copy(
                stage.at[slot, :, q * LANES : (q + 1) * LANES],
                out.at[m, span, q, :],
                sems.at[slot, q],
            )
            for q in range(pieces)
        ]

    row_at = lax.broadcasted_iota(jnp.int32, (LANES, LANES), 0)
    lane_at = lax.broadcasted_iota(jnp.int32, (LANES, LANES), 1)

    @pl.loop(0, batch_n * blocks)
    def _(at):
        slot = lax.rem(at, slots)
        m = at // blocks
        block = lax.rem(at, blocks)
        span = pl.ds(pl.multiple_of(block * LANES, LANES), LANES)

        @pl.when(at >= slots)
        def _():
            for copy in copies(at - slots):
                copy.wait()

        for q in range(0, pieces, 2):
            cut = slice(q * LANES, (q + 2) * LANES)
            change = jnp.dot(left[m, span, :], right[m, :, cut], preferred_element_type=F32)
            stage[slot, :, cut] = mats[m, span, cut] - change

        @pl.when(col_place == 0)
        def _():
            stage[slot, :, 0:LANES] = jnp.where(lane_at < TOTAL, 0.0, stage[slot, :, 0:LANES])

        @pl.when((row_place == 0) & (block == 0))
        def _():
            stage[slot, 0:ROWS_KEPT, :] = jnp.where(
                lax.broadcasted_iota(jnp.int32, (ROWS_KEPT, width), 0) < TOTAL,
                0.0,
                stage[slot, 0:ROWS_KEPT, :],
            )

        for copy in copies(at):
            copy.start()

    for at in range(batch_n * blocks - slots, batch_n * blocks):
        for copy in copies(at):
            copy.wait()


def update_all(mats, vx, yu, bid):
    batch_n, height, width = mats.shape
    pieces = width // LANES
    whole = pl.BlockSpec(memory_space=pltpu.VMEM)
    slots = 4
    return pl.pallas_call(
        update_kernel,
        out_shape=(
            jax.ShapeDtypeStruct((batch_n, height, pieces, LANES), F32),
            jax.ShapeDtypeStruct((batch_n, TOTAL), F32),
            jax.ShapeDtypeStruct((batch_n, TOTAL), F32),
        ),
        in_specs=[whole, whole, whole, whole],
        out_specs=(pl.BlockSpec(memory_space=pltpu.HBM), whole, whole),
        scratch_shapes=[
            pltpu.VMEM((batch_n, height, LANES), jnp.bfloat16),
            pltpu.VMEM((batch_n, LANES, width), jnp.bfloat16),
            pltpu.VMEM((slots, LANES, width), F32),
            pltpu.SemaphoreType.DMA((slots, pieces)),
        ],
        compiler_params=pltpu.CompilerParams(vmem_limit_bytes=24 * 1024 * 1024),
    )(mats, vx, yu, bid)


def per_device(weights):
    batch_n, row_cycles, tile_len, col_cycles, _ = weights.shape
    height = row_cycles * tile_len
    parts = tile_len // LANES
    row_n = lax.axis_size("row")
    col_n = lax.axis_size("col")
    w = weights.reshape(batch_n, row_cycles, tile_len, col_cycles, parts, LANES)
    w = w.transpose(0, 1, 2, 4, 3, 5).reshape(batch_n, height, parts * col_cycles, LANES)
    mats, vx, yu, bid = factor_all(w, row_n, col_n, tile_len)
    out, diagonal, superdiag = update_all(mats, vx, yu, bid)
    out = out.reshape(batch_n, row_cycles, tile_len, parts, col_cycles, LANES)
    trailing = out.transpose(0, 1, 2, 4, 3, 5).reshape(weights.shape)
    return (trailing, diagonal, superdiag)


def solution(mesh):
    placed = (P(None, None, "row", None, "col"),)
    return jax.shard_map(
        per_device,
        mesh=mesh,
        in_specs=placed,
        out_specs=(P(None, None, "row", None, "col"), P(), P()),
        check_vma=False,
    )
```

```python
import functools

import jax
import jax.numpy as jnp
from jax import lax
from jax.experimental import pallas as pl
from jax.experimental.pallas import tpu as pltpu
from jax.sharding import PartitionSpec as P

STEPS = 6
PANELS = 2
TOTAL = STEPS * PANELS
SLOTS = 2 * TOTAL
LANES = 128
SUB = 8
ROWS_KEPT = 16
MESH = pl.DeviceIdType.MESH
F32 = jnp.float32


def reflect(leading, squares):
    length = jnp.sqrt(squares)
    divisor = jnp.maximum(leading + length, 1.0)
    factor = (leading + length) / jnp.maximum(length, 1.0)
    return (divisor, factor, -length)


def partner(me, d, count):
    if count & (count - 1):
        return lax.rem(me + d, count), lax.rem(me - d + count, count)
    to = me
    bit = 1
    while bit < count:
        if d & bit:
            to = to + bit - 2 * bit * lax.rem(me // bit, 2)
        bit *= 2
    return to, to


def peers(axis, count):
    me = lax.axis_index(axis)
    return [partner(me, d, count) for d in range(count - 1, 0, -1)]


def row_ids(blocks, tile_len, devices, place):
    at = lax.broadcasted_iota(jnp.int32, (blocks, LANES), 0) * LANES
    at = at + lax.broadcasted_iota(jnp.int32, (blocks, LANES), 1)
    return at // tile_len * (devices * tile_len) + place * tile_len + at % tile_len


def col_ids(pieces, tile_len, devices, place):
    cycles = pieces * LANES // tile_len
    q = lax.broadcasted_iota(jnp.int32, (pieces, LANES), 0)
    lane = lax.broadcasted_iota(jnp.int32, (pieces, LANES), 1)
    return q % cycles * (devices * tile_len) + place * tile_len + q // cycles * LANES + lane


def tree(parts):
    while len(parts) > 1:
        parts = [
            parts[i] + parts[i + 1] if i + 1 < len(parts) else parts[i]
            for i in range(0, len(parts), 2)
        ]
    return parts[0]


def put_row(ref, m, at, dense, first=0):
    span = pl.ds(pl.multiple_of(at // SUB * SUB, SUB), SUB)
    here = lax.broadcasted_iota(jnp.int32, (SUB, LANES), 0) == lax.rem(at, SUB)
    for q in range(dense.shape[0]):
        cut = slice((first + q) * LANES, (first + q + 1) * LANES)
        ref[m, span, cut] = jnp.where(here, dense[q : q + 1], ref[m, span, cut])


def small_row(dots, picks, squares, leading):
    at = lax.broadcasted_iota(jnp.int32, (SUB, LANES), 0)
    extra = jnp.where(at == 0, squares, jnp.where(at == 1, leading, 0.0))
    rest = jnp.zeros((LANES - 2 * SLOTS - SUB, LANES), F32)
    tile = jnp.concatenate([dots, picks, extra, rest], axis=0)
    return jnp.sum(tile.T, axis=0, keepdims=True)


def kernel(
    row_n, col_n, tile_len, w, mats, vx, yu, bid,
    cols, rows, spread, sums, cd, rd, base_c, base_r, row_big, row_small, col_big, col_small,
    load_sem, rows_sem, row_send, row_recv, col_send, col_recv,
    first_send, first_recv, cols_send, cols_recv, rows_send, rows_recv,
):
    batch_n, height, pieces, _ = w.shape
    blocks = height // LANES
    row_place = lax.axis_index("row")
    col_place = lax.axis_index("col")
    row_peers = peers("row", row_n)
    col_peers = peers("col", col_n)

    def load(m, q):
        return pltpu.make_async_copy(
            w.at[m, :, q, :], mats.at[m, :, q * LANES : (q + 1) * LANES], load_sem.at[m, min(q, 1)]
        )

    def load_rows(m):
        return pltpu.make_async_copy(w.at[m, pl.ds(0, ROWS_KEPT)], rows.at[m], rows_sem.at[m])

    for m in range(batch_n):
        load(m, 0).start()

    @pl.when(row_place == 0)
    def _():
        for m in range(batch_n):
            load_rows(m).start()

    for m in range(batch_n):
        for q in range(1, pieces):
            load(m, q).start()

    vx[...] = jnp.zeros_like(vx)
    yu[...] = jnp.zeros_like(yu)
    bid[...] = jnp.zeros_like(bid)
    rd[...] = jnp.zeros_like(rd)
    col_big[...] = jnp.zeros_like(col_big)
    col_small[...] = jnp.zeros_like(col_small)

    barrier = pltpu.get_barrier_semaphore()
    for axis, count, others in (("row", row_n, row_peers), ("col", col_n, col_peers)):
        for to, _ in others:
            pl.semaphore_signal(barrier, inc=1, device_id={axis: to}, device_id_type=MESH)
    pl.semaphore_wait(barrier, row_n + col_n - 2)

    def remote(ref, send, recv, axis, to):
        return pltpu.make_async_remote_copy(
            src_ref=ref,
            dst_ref=ref,
            send_sem=send,
            recv_sem=recv,
            device_id={axis: to},
            device_id_type=MESH,
        )

    def first_col(at, to):
        return remote(cols.at[:, 0], first_send.at[at], first_recv, "col", to)

    def later_cols(at, to):
        return remote(
            cols.at[:, pl.ds(1, TOTAL)], cols_send.at[at], cols_recv, "col", to
        )

    def row_copy(m, k, at, to):
        return remote(rows.at[m, k], rows_send.at[m, at], rows_recv.at[m, k], "row", to)

    for m in range(batch_n):
        load(m, 0).wait()

    @pl.when(col_place == 0)
    def _():
        for m in range(batch_n):
            for b in range(blocks):
                turned = mats[m, b * LANES : (b + 1) * LANES, 0:LANES].T
                for j in range(TOTAL + 1):
                    cols[m, j, b : b + 1, :] = turned[j : j + 1]
        for at, (to, _) in enumerate(col_peers):
            first_col(at, to).start()
        for at, (to, _) in enumerate(col_peers):
            later_cols(at, to).start()

    @pl.when(row_place == 0)
    def _():
        for m in range(batch_n):
            load_rows(m).wait()
            for at, (to, _) in enumerate(row_peers):
                row_copy(m, 0, at, to).start()

    @pl.when(col_place != 0)
    def _():
        first_col(0, 0).wait_recv()

    grow = row_ids(blocks, tile_len, row_n, row_place)
    gcol = col_ids(pieces, tile_len, col_n, col_place)
    lane = lax.broadcasted_iota(jnp.int32, (1, LANES), 1)
    own_row = jnp.where(row_place == 0, lane, -1)
    own_col = jnp.where(col_place == 0, lane, -1)
    row_at = lax.broadcasted_iota(jnp.int32, (SUB, LANES), 0)
    lane_at = lax.broadcasted_iota(jnp.int32, (SUB, LANES), 1)

    half = pieces // 2

    def channel(axis, par, m, which):
        me = lax.axis_index(axis)
        small, big, sems, others = (
            (row_small, row_big, (row_send, row_recv), row_peers)
            if axis == "row"
            else (col_small, col_big, (col_send, col_recv), col_peers)
        )
        ref = small.at[par, m] if which == 0 else big.at[par, m, which - 1]
        own = ref.at[pl.ds(me, 1)]
        every = ref.at[pl.ds(0, len(others))]
        return own, every, (sems[0].at[m, which], sems[1].at[par, m, which]), others

    def post(axis, par, m, which):
        own, _, sems, others = channel(axis, par, m, which)
        for to, _ in others:
            remote(own, *sems, axis, to).start()

    def take(axis, par, m, which):
        _, every, sems, others = channel(axis, par, m, which)
        remote(every, *sems, axis, others[0][0]).wait_recv()

    def sent(axis, par, m, count):
        for which in range(count):
            _, every, sems, others = channel(axis, par, m, which)
            remote(every, *sems, axis, others[0][0]).wait_send()

    def sums_of(ref, par, m):
        total = jnp.sum(ref[par, m], axis=0, keepdims=True)
        turned = jnp.broadcast_to(total, (LANES, LANES)).T
        dots = turned[0:SLOTS]
        picks = turned[SLOTS : 2 * SLOTS]
        squares = turned[2 * SLOTS : 2 * SLOTS + 1]
        leading = turned[2 * SLOTS + 1 : 2 * SLOTS + 2]
        divisor, factor, bidiag = reflect(leading, squares)
        remain = 1.0 - leading / divisor
        weight = dots / divisor + picks * remain
        return divisor, factor, bidiag, remain, weight, picks

    def before_col(k, m):
        par = lax.rem(k + 1, 2)

        @pl.when(k > 0)
        def _():
            sent("row", par, m, 3)
            take("col", par, m, 0)

        divisor, factor, bidiag, remain, weight, picks = sums_of(col_small, par, m)
        bid[1] = jnp.where((row_at == m) & (lane_at == k - 1), bidiag, bid[1])
        row_vec = jnp.where(gcol == k, 1.0, rd[m] / divisor)
        row_vec = jnp.where(k > 0, row_vec, 0.0)
        at = jnp.where(k > 0, TOTAL - 1 + k, 0)
        put_row(yu, m, at, row_vec)
        column = cols[m, k]
        for b in range(blocks):
            old = vx[m, :, b * LANES : (b + 1) * LANES]
            base_c[m, 0, b : b + 1, :] = factor * (
                column[b : b + 1] * remain - jnp.sum(weight * old, axis=0, keepdims=True)
            )
            base_c[m, 1, b : b + 1, :] = column[b : b + 1] - jnp.sum(
                picks * old, axis=0, keepdims=True
            )
        base_c[m, 2] = jnp.broadcast_to(factor / divisor, (blocks, LANES))

    def new_col(k, m):
        par = lax.rem(k + 1, 2)

        @pl.when(k > 0)
        def _():
            take("col", par, m, 1)

        applied = tree([col_big[par, m, 0, s] for s in range(col_n)])
        image = jnp.where(grow >= k, base_c[m, 2] * applied + base_c[m, 0], 0.0)
        at = jnp.where(k > 0, TOTAL - 1 + k, 0)
        put_row(vx, m, at, image)
        return image

    def col_half(k, m):
        par = lax.rem(k, 2)
        image = new_col(k, m)
        piece = jnp.where(grow >= k, base_c[m, 1] - image, 0.0)
        cd[m] = piece

        def fill(b):
            spread[b * LANES : (b + 1) * LANES, :] = jnp.broadcast_to(
                cd[m, b : b + 1, :], (LANES, LANES)
            ).T

        fill(0)
        dots = tree(
            [
                vx[m, :, b * LANES : (b + 1) * LANES] * piece[b : b + 1]
                for b in range(blocks)
            ]
        )
        picks = jnp.where(own_row == k, vx[m, :, 0:LANES], 0.0)
        squares = jnp.sum(piece * piece, axis=0, keepdims=True)
        leading = jnp.sum(jnp.where(grow == k, piece, 0.0), axis=0, keepdims=True)
        small = small_row(dots, picks, squares, leading)
        for b in range(1, blocks):
            fill(b)
        for part in range(2):
            total = [None] * half
            for b in range(blocks):
                for g in range(LANES // SUB):
                    span = pl.ds(b * LANES + g * SUB, SUB)
                    by = spread[span, :]
                    for q in range(half):
                        at = (part * half + q) * LANES
                        term = mats[m, span, at : at + LANES] * by
                        total[q] = term if total[q] is None else total[q] + term
                if part == 0 and b == blocks // 2 - 1:
                    row_small[par, m, pl.ds(row_place, 1), :] = small
                    post("row", par, m, 0)
            for q in range(half):
                row_big[par, m, part, row_place, q : q + 1, :] = jnp.sum(
                    total[q], axis=0, keepdims=True
                )
            post("row", par, m, 1 + part)

        @pl.when((row_place == 0) & (k < TOTAL - 1))
        def _():
            for at, (to, _) in enumerate(row_peers):
                row_copy(m, k, at, to).wait_send()
            for at, (to, _) in enumerate(row_peers):
                row_copy(m, k + 1, at, to).start()

    def before_row(k, m):
        par = lax.rem(k, 2)
        @pl.when(k > 0)
        def _():
            sent("col", par, m, 2)

        take("row", par, m, 0)

        @pl.when(row_place != 0)
        def _():
            row_copy(m, k, 0, 0).wait_recv()

        divisor, factor, bidiag, remain, weight, picks = sums_of(row_small, par, m)
        bid[0] = jnp.where((row_at == m) & (lane_at == k), bidiag, bid[0])
        col_vec = jnp.where(grow == k, 1.0, cd[m] / divisor)
        put_row(vx, m, k, col_vec)
        row = rows[m, k]
        for q in range(pieces):
            old = yu[m, :, q * LANES : (q + 1) * LANES]
            base_r[m, 0, q : q + 1, :] = factor * (
                row[q : q + 1] * remain - jnp.sum(weight * old, axis=0, keepdims=True)
            )
            base_r[m, 1, q : q + 1, :] = row[q : q + 1] - jnp.sum(
                picks * old, axis=0, keepdims=True
            )
        base_r[m, 2] = jnp.broadcast_to(factor / divisor, (pieces, LANES))

    def row_half(k, m):
        par = lax.rem(k, 2)
        dots = squares = leading = None
        for part in range(2):
            tiles = slice(part * half, (part + 1) * half)
            take("row", par, m, 1 + part)
            trans = tree([row_big[par, m, part, s] for s in range(row_n)])
            here = gcol[tiles]
            image = jnp.where(here > k, base_r[m, 2, tiles] * trans + base_r[m, 0, tiles], 0.0)
            put_row(yu, m, k, image, part * half)
            piece = jnp.where(here > k, base_r[m, 1, tiles] - image, 0.0)
            rd[m, tiles] = piece
            terms = [
                yu[m, :, (part * half + q) * LANES : (part * half + q + 1) * LANES]
                * piece[q : q + 1]
                for q in range(half)
            ]
            dots = tree(terms if part == 0 else [dots] + terms)
            square = jnp.sum(piece * piece, axis=0, keepdims=True)
            lead = jnp.sum(jnp.where(here == k + 1, piece, 0.0), axis=0, keepdims=True)
            squares = square if part == 0 else squares + square
            leading = lead if part == 0 else leading + lead
            if part == 1:
                picks = jnp.where(own_col == k + 1, yu[m, :, 0:LANES], 0.0)
                small = small_row(dots, picks, squares, leading)
            scale = [
                jnp.broadcast_to(rd[m, part * half + q : part * half + q + 1, :], (SUB, LANES))
                for q in range(half)
            ]
            for b in range(blocks):
                groups = []
                for g in range(LANES // SUB):
                    span = pl.ds(b * LANES + g * SUB, SUB)
                    products = []
                    for q in range(half):
                        at = (part * half + q) * LANES
                        products.append(mats[m, span, at : at + LANES] * scale[q])
                    if part == 0:
                        sums[span, :] = tree(products)
                    else:
                        groups.append(tree(products) + sums[span, :])
                if part == 1:
                    turned = jnp.concatenate(groups, axis=0).T
                    col_big[par, m, 0, col_place, b : b + 1, :] = jnp.sum(
                        turned, axis=0, keepdims=True
                    )
                    if b == min(2, blocks - 1):
                        col_small[par, m, pl.ds(col_place, 1), :] = small
                        post("col", par, m, 0)
        post("col", par, m, 1)

    def step_body(k, carry):
        for m in range(batch_n):

            @pl.when(k == 0)
            def _():
                rest = mats.at[m, :, LANES:]
                pltpu.make_async_copy(rest, rest, load_sem.at[m, 1]).wait()

            before_col(k, m)
            col_half(k, m)
        for m in range(batch_n):
            before_row(k, m)
            row_half(k, m)

        @pl.when((k == 0) & (col_place != 0))
        def _():
            later_cols(0, 0).wait_recv()

        return carry

    lax.fori_loop(0, TOTAL, step_body, 0)
    for m in range(batch_n):
        before_col(TOTAL, m)
        new_col(TOTAL, m)
        sent("col", (TOTAL + 1) % 2, m, 2)

    @pl.when(col_place == 0)
    def _():
        for at, (to, _) in enumerate(col_peers):
            first_col(at, to).wait_send()
            later_cols(at, to).wait_send()

    @pl.when(row_place == 0)
    def _():
        for m in range(batch_n):
            for at, (to, _) in enumerate(row_peers):
                row_copy(m, TOTAL - 1, at, to).wait_send()


def factor_all(w, row_n, col_n, tile_len):
    batch_n, height, pieces, _ = w.shape
    width = pieces * LANES
    blocks = height // LANES
    whole = pl.BlockSpec(memory_space=pltpu.VMEM)
    return pl.pallas_call(
        functools.partial(kernel, row_n, col_n, tile_len),
        out_shape=(
            jax.ShapeDtypeStruct((batch_n, height, width), F32),
            jax.ShapeDtypeStruct((batch_n, SLOTS, height), F32),
            jax.ShapeDtypeStruct((batch_n, SLOTS, width), F32),
            jax.ShapeDtypeStruct((2, SUB, LANES), F32),
        ),
        in_specs=[pl.BlockSpec(memory_space=pltpu.HBM)],
        out_specs=(whole, whole, whole, whole),
        scratch_shapes=[
            pltpu.VMEM((batch_n, TOTAL + 1, blocks, LANES), F32),
            pltpu.VMEM((batch_n, ROWS_KEPT, pieces, LANES), F32),
            pltpu.VMEM((height, LANES), F32),
            pltpu.VMEM((height, LANES), F32),
            pltpu.VMEM((batch_n, blocks, LANES), F32),
            pltpu.VMEM((batch_n, pieces, LANES), F32),
            pltpu.VMEM((batch_n, 3, blocks, LANES), F32),
            pltpu.VMEM((batch_n, 3, pieces, LANES), F32),
            pltpu.VMEM((2, batch_n, 2, row_n, pieces // 2, LANES), F32),
            pltpu.VMEM((2, batch_n, row_n, LANES), F32),
            pltpu.VMEM((2, batch_n, 1, col_n, blocks, LANES), F32),
            pltpu.VMEM((2, batch_n, col_n, LANES), F32),
            pltpu.SemaphoreType.DMA((batch_n, 2)),
            pltpu.SemaphoreType.DMA((batch_n,)),
            pltpu.SemaphoreType.DMA((batch_n, 3)),
            pltpu.SemaphoreType.DMA((2, batch_n, 3)),
            pltpu.SemaphoreType.DMA((batch_n, 2)),
            pltpu.SemaphoreType.DMA((2, batch_n, 2)),
            pltpu.SemaphoreType.DMA((col_n,)),
            pltpu.SemaphoreType.DMA,
            pltpu.SemaphoreType.DMA((col_n,)),
            pltpu.SemaphoreType.DMA,
            pltpu.SemaphoreType.DMA((batch_n, row_n)),
            pltpu.SemaphoreType.DMA((batch_n, TOTAL)),
        ],
        compiler_params=pltpu.CompilerParams(
            collective_id=0, has_side_effects=True, vmem_limit_bytes=24 * 1024 * 1024
        ),
    )(w)


def update_kernel(mats, vx, yu, bid, out, diagonal, superdiag, left, right, stage, sems):
    batch_n, height, width = mats.shape
    pieces = width // LANES
    blocks = height // LANES
    row_place = lax.axis_index("row")
    col_place = lax.axis_index("col")
    slots = stage.shape[0]
    diagonal[...] = bid[0, 0:batch_n, 0:TOTAL]
    superdiag[...] = bid[1, 0:batch_n, 0:TOTAL]
    empty = jnp.zeros((LANES - 4 * SLOTS, LANES), F32)

    def halves(value):
        high = value.astype(jnp.bfloat16).astype(F32)
        return high, value - high

    def put_left(m, b):
        span = pl.ds(pl.multiple_of(b * LANES, LANES), LANES)
        high, low = halves(vx[m, :, span])
        stack = jnp.concatenate([high, high, low, low, empty], axis=0)
        left[lax.rem(b, 2)] = stack.T.astype(jnp.bfloat16)

    def put_right(m):
        for q in range(pieces):
            high, low = halves(yu[m, :, q * LANES : (q + 1) * LANES])
            stack = jnp.concatenate([high, low, high, low, empty], axis=0)
            right[:, q * LANES : (q + 1) * LANES] = stack.astype(jnp.bfloat16)

    def copies(at):
        slot = lax.rem(at, slots)
        m = at // blocks
        span = pl.ds(pl.multiple_of(lax.rem(at, blocks) * LANES, LANES), LANES)
        return [
            pltpu.make_async_copy(
                stage.at[slot, :, q * LANES : (q + 1) * LANES],
                out.at[m, span, q, :],
                sems.at[slot],
            )
            for q in range(pieces)
        ]

    def drain(at):
        slot = lax.rem(at, slots)
        pltpu.make_async_copy(stage.at[slot], stage.at[slot], sems.at[slot]).wait()

    lane_at = lax.broadcasted_iota(jnp.int32, (LANES, LANES), 1)

    def block_body(m, block):
        at = m * blocks + block
        slot = lax.rem(at, slots)
        span = pl.ds(pl.multiple_of(block * LANES, LANES), LANES)

        @pl.when(at >= slots)
        def _():
            drain(at)

        for q in range(0, pieces, 2):
            cut = slice(q * LANES, (q + 2) * LANES)
            change = jnp.dot(
                left[lax.rem(block, 2)], right[:, cut], preferred_element_type=F32
            )
            stage[slot, :, cut] = mats[m, span, cut] - change

        put_left(m, lax.rem(block + 1, blocks))

        @pl.when(col_place == 0)
        def _():
            stage[slot, :, 0:LANES] = jnp.where(lane_at < TOTAL, 0.0, stage[slot, :, 0:LANES])

        @pl.when((row_place == 0) & (block == 0))
        def _():
            stage[slot, 0:ROWS_KEPT, :] = jnp.where(
                lax.broadcasted_iota(jnp.int32, (ROWS_KEPT, width), 0) < TOTAL,
                0.0,
                stage[slot, 0:ROWS_KEPT, :],
            )

        for copy in copies(at):
            copy.start()

    for m in range(batch_n):
        put_left(m, 0)
        put_right(m)
        pl.loop(0, blocks)(functools.partial(block_body, m))

    for at in range(batch_n * blocks - slots, batch_n * blocks):
        drain(at)


def update_all(mats, vx, yu, bid):
    batch_n, height, width = mats.shape
    pieces = width // LANES
    whole = pl.BlockSpec(memory_space=pltpu.VMEM)
    slots = min(4, batch_n * height // LANES)
    return pl.pallas_call(
        update_kernel,
        out_shape=(
            jax.ShapeDtypeStruct((batch_n, height, pieces, LANES), F32),
            jax.ShapeDtypeStruct((batch_n, TOTAL), F32),
            jax.ShapeDtypeStruct((batch_n, TOTAL), F32),
        ),
        in_specs=[whole, whole, whole, whole],
        out_specs=(pl.BlockSpec(memory_space=pltpu.HBM), whole, whole),
        scratch_shapes=[
            pltpu.VMEM((2, LANES, LANES), jnp.bfloat16),
            pltpu.VMEM((LANES, width), jnp.bfloat16),
            pltpu.VMEM((slots, LANES, width), F32),
            pltpu.SemaphoreType.DMA((slots,)),
        ],
        compiler_params=pltpu.CompilerParams(vmem_limit_bytes=24 * 1024 * 1024),
    )(mats, vx, yu, bid)


def per_device(weights):
    batch_n, row_cycles, tile_len, col_cycles, _ = weights.shape
    height = row_cycles * tile_len
    parts = tile_len // LANES
    row_n = lax.axis_size("row")
    col_n = lax.axis_size("col")
    w = weights.reshape(batch_n, row_cycles, tile_len, col_cycles, parts, LANES)
    w = w.transpose(0, 1, 2, 4, 3, 5).reshape(batch_n, height, parts * col_cycles, LANES)
    mats, vx, yu, bid = factor_all(w, row_n, col_n, tile_len)
    out, diagonal, superdiag = update_all(mats, vx, yu, bid)
    out = out.reshape(batch_n, row_cycles, tile_len, parts, col_cycles, LANES)
    trailing = out.transpose(0, 1, 2, 4, 3, 5).reshape(weights.shape)
    return (trailing, diagonal, superdiag)


def solution(mesh):
    placed = (P(None, None, "row", None, "col"),)
    return jax.shard_map(
        per_device,
        mesh=mesh,
        in_specs=placed,
        out_specs=(P(None, None, "row", None, "col"), P(), P()),
        check_vma=False,
    )
```

```python
import functools

import jax
import jax.numpy as jnp
from jax import lax
from jax.experimental import pallas as pl
from jax.experimental.pallas import tpu as pltpu
from jax.sharding import PartitionSpec as P

STEPS = 6
PANELS = 2
TOTAL = STEPS * PANELS
SLOTS = 2 * TOTAL
LANES = 128
SUB = 8
ROWS_KEPT = 16
MESH = pl.DeviceIdType.MESH
F32 = jnp.float32


def reflect(leading, squares):
    length = jnp.sqrt(squares)
    divisor = jnp.maximum(leading + length, 1.0)
    factor = (leading + length) / jnp.maximum(length, 1.0)
    return (divisor, factor, -length)


def partner(me, d, count):
    if count & (count - 1):
        return lax.rem(me + d, count), lax.rem(me - d + count, count)
    to = me
    bit = 1
    while bit < count:
        if d & bit:
            to = to + bit - 2 * bit * lax.rem(me // bit, 2)
        bit *= 2
    return to, to


def peers(axis, count):
    me = lax.axis_index(axis)
    return [partner(me, d, count) for d in range(count - 1, 0, -1)]


def row_ids(blocks, tile_len, devices, place):
    at = lax.broadcasted_iota(jnp.int32, (blocks, LANES), 0) * LANES
    at = at + lax.broadcasted_iota(jnp.int32, (blocks, LANES), 1)
    return at // tile_len * (devices * tile_len) + place * tile_len + at % tile_len


def col_ids(pieces, tile_len, devices, place):
    cycles = pieces * LANES // tile_len
    q = lax.broadcasted_iota(jnp.int32, (pieces, LANES), 0)
    lane = lax.broadcasted_iota(jnp.int32, (pieces, LANES), 1)
    return q % cycles * (devices * tile_len) + place * tile_len + q // cycles * LANES + lane


def tree(parts):
    while len(parts) > 1:
        parts = [
            parts[i] + parts[i + 1] if i + 1 < len(parts) else parts[i]
            for i in range(0, len(parts), 2)
        ]
    return parts[0]


def put_row(ref, m, at, dense, first=0):
    span = pl.ds(pl.multiple_of(at // SUB * SUB, SUB), SUB)
    here = lax.broadcasted_iota(jnp.int32, (SUB, LANES), 0) == lax.rem(at, SUB)
    for q in range(dense.shape[0]):
        cut = slice((first + q) * LANES, (first + q + 1) * LANES)
        ref[m, span, cut] = jnp.where(here, dense[q : q + 1], ref[m, span, cut])


def small_row(dots, picks, squares, leading):
    at = lax.broadcasted_iota(jnp.int32, (SUB, LANES), 0)
    extra = jnp.where(at == 0, squares, jnp.where(at == 1, leading, 0.0))
    rest = jnp.zeros((LANES - 2 * SLOTS - SUB, LANES), F32)
    tile = jnp.concatenate([dots, picks, extra, rest], axis=0)
    return jnp.sum(tile.T, axis=0, keepdims=True)


def kernel(
    row_n, col_n, tile_len, w, mats, vx, yu, bid,
    cols, rows, spread, sums, cd, rd, base_c, base_r, row_big, row_small, col_big, col_small,
    load_sem, rows_sem, row_send, row_recv, col_send, col_recv,
    first_send, first_recv, cols_send, cols_recv, rows_send, rows_recv,
):
    batch_n, height, pieces, _ = w.shape
    blocks = height // LANES
    row_place = lax.axis_index("row")
    col_place = lax.axis_index("col")
    row_peers = peers("row", row_n)
    col_peers = peers("col", col_n)

    def load(m, q):
        return pltpu.make_async_copy(
            w.at[m, :, q, :], mats.at[m, :, q * LANES : (q + 1) * LANES], load_sem.at[m, min(q, 1)]
        )

    def load_rows(m):
        return pltpu.make_async_copy(w.at[m, pl.ds(0, ROWS_KEPT)], rows.at[m], rows_sem.at[m])

    for m in range(batch_n):
        load(m, 0).start()

    @pl.when(row_place == 0)
    def _():
        for m in range(batch_n):
            load_rows(m).start()

    for m in range(batch_n):
        for q in range(1, pieces):
            load(m, q).start()

    vx[...] = jnp.zeros_like(vx)
    yu[...] = jnp.zeros_like(yu)
    bid[...] = jnp.zeros_like(bid)
    rd[...] = jnp.zeros_like(rd)
    col_big[...] = jnp.zeros_like(col_big)
    col_small[...] = jnp.zeros_like(col_small)

    barrier = pltpu.get_barrier_semaphore()
    for axis, count, others in (("row", row_n, row_peers), ("col", col_n, col_peers)):
        for to, _ in others:
            pl.semaphore_signal(barrier, inc=1, device_id={axis: to}, device_id_type=MESH)
    pl.semaphore_wait(barrier, row_n + col_n - 2)

    def remote(ref, send, recv, axis, to):
        return pltpu.make_async_remote_copy(
            src_ref=ref,
            dst_ref=ref,
            send_sem=send,
            recv_sem=recv,
            device_id={axis: to},
            device_id_type=MESH,
        )

    def first_col(at, to):
        return remote(cols.at[:, 0], first_send.at[at], first_recv, "col", to)

    def later_cols(at, to):
        return remote(
            cols.at[:, pl.ds(1, TOTAL)], cols_send.at[at], cols_recv, "col", to
        )

    def row_copy(m, k, to):
        return remote(rows.at[m, k], rows_send.at[m], rows_recv.at[m, k], "row", to)

    def rows_sent(m):
        every = row_big.at[0, 0, pl.ds(0, 2), pl.ds(0, row_n - 1)]
        remote(every, rows_send.at[m], rows_recv.at[m, 0], "row", row_peers[0][0]).wait_send()

    for m in range(batch_n):
        load(m, 0).wait()

    @pl.when(col_place == 0)
    def _():
        for m in range(batch_n):
            for b in range(blocks):
                turned = mats[m, b * LANES : (b + 1) * LANES, 0:LANES].T
                cols[m, 0, b : b + 1, :] = turned[0:1]
                spread[(m * blocks + b) * SUB : (m * blocks + b + 1) * SUB, :] = turned[0:SUB]
                sums[(m * blocks + b) * SUB : (m * blocks + b + 1) * SUB, :] = turned[SUB : 2 * SUB]
        for at, (to, _) in enumerate(col_peers):
            first_col(at, to).start()
        for m in range(batch_n):
            for b in range(blocks):
                for j in range(1, TOTAL + 1):
                    held = spread if j < SUB else sums
                    at = (m * blocks + b) * SUB + j % SUB
                    cols[m, j, b : b + 1, :] = held[at : at + 1, :]
        for at, (to, _) in enumerate(col_peers):
            later_cols(at, to).start()

    @pl.when(row_place == 0)
    def _():
        for m in range(batch_n):
            load_rows(m).wait()
            for to, _ in row_peers:
                row_copy(m, 0, to).start()

    @pl.when(col_place != 0)
    def _():
        first_col(0, 0).wait_recv()

    grow = row_ids(blocks, tile_len, row_n, row_place)
    gcol = col_ids(pieces, tile_len, col_n, col_place)
    lane = lax.broadcasted_iota(jnp.int32, (1, LANES), 1)
    own_row = jnp.where(row_place == 0, lane, -1)
    own_col = jnp.where(col_place == 0, lane, -1)
    row_at = lax.broadcasted_iota(jnp.int32, (SUB, LANES), 0)
    lane_at = lax.broadcasted_iota(jnp.int32, (SUB, LANES), 1)

    half = pieces // 2

    def channel(axis, par, m, which):
        me = lax.axis_index(axis)
        small, big, sems, others = (
            (row_small, row_big, (row_send, row_recv), row_peers)
            if axis == "row"
            else (col_small, col_big, (col_send, col_recv), col_peers)
        )
        ref = small.at[par, m] if which == 0 else big.at[par, m, which - 1]
        own = ref.at[pl.ds(me, 1)]
        every = ref.at[pl.ds(0, len(others))]
        return own, every, (sems[0].at[m, which], sems[1].at[par, m, which]), others

    def post(axis, par, m, which):
        own, _, sems, others = channel(axis, par, m, which)
        for to, _ in others:
            remote(own, *sems, axis, to).start()

    def take(axis, par, m, which):
        _, every, sems, others = channel(axis, par, m, which)
        remote(every, *sems, axis, others[0][0]).wait_recv()

    def sent(axis, par, m, count):
        for which in range(count):
            _, every, sems, others = channel(axis, par, m, which)
            remote(every, *sems, axis, others[0][0]).wait_send()

    def sums_of(ref, par, m):
        total = jnp.sum(ref[par, m], axis=0, keepdims=True)
        turned = jnp.broadcast_to(total, (LANES, LANES)).T
        dots = turned[0:SLOTS]
        picks = turned[SLOTS : 2 * SLOTS]
        squares = turned[2 * SLOTS : 2 * SLOTS + 1]
        leading = turned[2 * SLOTS + 1 : 2 * SLOTS + 2]
        divisor, factor, bidiag = reflect(leading, squares)
        remain = 1.0 - leading / divisor
        weight = dots / divisor + picks * remain
        return divisor, factor, bidiag, remain, weight, picks

    def before_col(k, m):
        par = lax.rem(k + 1, 2)

        @pl.when(k > 0)
        def _():
            sent("row", par, m, 3)
            take("col", par, m, 0)

        divisor, factor, bidiag, remain, weight, picks = sums_of(col_small, par, m)
        bid[1] = jnp.where((row_at == m) & (lane_at == k - 1), bidiag, bid[1])
        row_vec = jnp.where(gcol == k, 1.0, rd[m] / divisor)
        row_vec = jnp.where(k > 0, row_vec, 0.0)
        at = jnp.where(k > 0, TOTAL - 1 + k, 0)
        put_row(yu, m, at, row_vec)
        column = cols[m, k]
        for b in range(blocks):
            old = vx[m, :, b * LANES : (b + 1) * LANES]
            base_c[m, 0, b : b + 1, :] = factor * (
                column[b : b + 1] * remain - jnp.sum(weight * old, axis=0, keepdims=True)
            )
            base_c[m, 1, b : b + 1, :] = column[b : b + 1] - jnp.sum(
                picks * old, axis=0, keepdims=True
            )
        base_c[m, 2] = jnp.broadcast_to(factor / divisor, (blocks, LANES))

    def new_col(k, m):
        par = lax.rem(k + 1, 2)

        @pl.when(k > 0)
        def _():
            take("col", par, m, 1)

        applied = tree([col_big[par, m, 0, s] for s in range(col_n)])
        image = jnp.where(grow >= k, base_c[m, 2] * applied + base_c[m, 0], 0.0)
        at = jnp.where(k > 0, TOTAL - 1 + k, 0)
        put_row(vx, m, at, image)
        return image

    def col_half(k, m):
        par = lax.rem(k, 2)
        image = new_col(k, m)
        piece = jnp.where(grow >= k, base_c[m, 1] - image, 0.0)
        cd[m] = piece

        def fill(b):
            spread[b * LANES : (b + 1) * LANES, :] = jnp.broadcast_to(
                cd[m, b : b + 1, :], (LANES, LANES)
            ).T

        fill(0)
        dots = tree(
            [
                vx[m, :, b * LANES : (b + 1) * LANES] * piece[b : b + 1]
                for b in range(blocks)
            ]
        )
        picks = jnp.where(own_row == k, vx[m, :, 0:LANES], 0.0)
        squares = jnp.sum(piece * piece, axis=0, keepdims=True)
        leading = jnp.sum(jnp.where(grow == k, piece, 0.0), axis=0, keepdims=True)
        small = small_row(dots, picks, squares, leading)
        for b in range(1, blocks):
            fill(b)
        for part in range(2):
            total = [None] * half
            for b in range(blocks):
                for g in range(LANES // SUB):
                    span = pl.ds(b * LANES + g * SUB, SUB)
                    by = spread[span, :]
                    for q in range(half):
                        at = (part * half + q) * LANES
                        term = mats[m, span, at : at + LANES] * by
                        total[q] = term if total[q] is None else total[q] + term
                if part == 0 and b == blocks // 2 - 1:
                    row_small[par, m, pl.ds(row_place, 1), :] = small
                    post("row", par, m, 0)
            for q in range(half):
                row_big[par, m, part, row_place, q : q + 1, :] = jnp.sum(
                    total[q], axis=0, keepdims=True
                )
            post("row", par, m, 1 + part)

    def before_row(k, m):
        par = lax.rem(k, 2)
        @pl.when(k > 0)
        def _():
            sent("col", par, m, 2)

        take("row", par, m, 0)

        @pl.when(row_place != 0)
        def _():
            row_copy(m, k, 0).wait_recv()

        divisor, factor, bidiag, remain, weight, picks = sums_of(row_small, par, m)
        bid[0] = jnp.where((row_at == m) & (lane_at == k), bidiag, bid[0])
        col_vec = jnp.where(grow == k, 1.0, cd[m] / divisor)
        put_row(vx, m, k, col_vec)
        row = rows[m, k]
        for q in range(pieces):
            old = yu[m, :, q * LANES : (q + 1) * LANES]
            base_r[m, 0, q : q + 1, :] = factor * (
                row[q : q + 1] * remain - jnp.sum(weight * old, axis=0, keepdims=True)
            )
            base_r[m, 1, q : q + 1, :] = row[q : q + 1] - jnp.sum(
                picks * old, axis=0, keepdims=True
            )
        base_r[m, 2] = jnp.broadcast_to(factor / divisor, (pieces, LANES))

    def row_half(k, m):
        par = lax.rem(k, 2)
        dots = squares = leading = None
        for part in range(2):
            tiles = slice(part * half, (part + 1) * half)
            take("row", par, m, 1 + part)
            trans = tree([row_big[par, m, part, s] for s in range(row_n)])
            here = gcol[tiles]
            image = jnp.where(here > k, base_r[m, 2, tiles] * trans + base_r[m, 0, tiles], 0.0)
            put_row(yu, m, k, image, part * half)
            piece = jnp.where(here > k, base_r[m, 1, tiles] - image, 0.0)
            rd[m, tiles] = piece
            terms = [
                yu[m, :, (part * half + q) * LANES : (part * half + q + 1) * LANES]
                * piece[q : q + 1]
                for q in range(half)
            ]
            dots = tree(terms if part == 0 else [dots] + terms)
            square = jnp.sum(piece * piece, axis=0, keepdims=True)
            lead = jnp.sum(jnp.where(here == k + 1, piece, 0.0), axis=0, keepdims=True)
            squares = square if part == 0 else squares + square
            leading = lead if part == 0 else leading + lead
            if part == 1:
                picks = jnp.where(own_col == k + 1, yu[m, :, 0:LANES], 0.0)
                small = small_row(dots, picks, squares, leading)
            scale = [
                jnp.broadcast_to(rd[m, part * half + q : part * half + q + 1, :], (SUB, LANES))
                for q in range(half)
            ]
            for b in range(blocks):
                groups = []
                for g in range(LANES // SUB):
                    span = pl.ds(b * LANES + g * SUB, SUB)
                    products = []
                    for q in range(half):
                        at = (part * half + q) * LANES
                        products.append(mats[m, span, at : at + LANES] * scale[q])
                    if part == 0:
                        sums[span, :] = tree(products)
                    else:
                        groups.append(tree(products) + sums[span, :])
                if part == 1:
                    turned = jnp.concatenate(groups, axis=0).T
                    col_big[par, m, 0, col_place, b : b + 1, :] = jnp.sum(
                        turned, axis=0, keepdims=True
                    )
                    if b == min(2, blocks - 1):
                        col_small[par, m, pl.ds(col_place, 1), :] = small
                        post("col", par, m, 0)
        post("col", par, m, 1)

    def step_body(k, carry):
        for m in range(batch_n):

            @pl.when(k == 0)
            def _():
                rest = mats.at[m, :, LANES:]
                pltpu.make_async_copy(rest, rest, load_sem.at[m, 1]).wait()

            before_col(k, m)
            col_half(k, m)

        @pl.when((row_place == 0) & (k < TOTAL - 1))
        def _():
            for m in range(batch_n):
                rows_sent(m)
                for to, _ in row_peers:
                    row_copy(m, k + 1, to).start()

        for m in range(batch_n):
            before_row(k, m)
            row_half(k, m)

        @pl.when((k == 0) & (col_place != 0))
        def _():
            later_cols(0, 0).wait_recv()

        return carry

    lax.fori_loop(0, TOTAL, step_body, 0)
    for m in range(batch_n):
        before_col(TOTAL, m)
        new_col(TOTAL, m)
        sent("col", (TOTAL + 1) % 2, m, 2)

    @pl.when(col_place == 0)
    def _():
        for at, (to, _) in enumerate(col_peers):
            first_col(at, to).wait_send()
            later_cols(at, to).wait_send()

    @pl.when(row_place == 0)
    def _():
        for m in range(batch_n):
            rows_sent(m)


def factor_all(w, row_n, col_n, tile_len):
    batch_n, height, pieces, _ = w.shape
    width = pieces * LANES
    blocks = height // LANES
    whole = pl.BlockSpec(memory_space=pltpu.VMEM)
    return pl.pallas_call(
        functools.partial(kernel, row_n, col_n, tile_len),
        out_shape=(
            jax.ShapeDtypeStruct((batch_n, height, width), F32),
            jax.ShapeDtypeStruct((batch_n, SLOTS, height), F32),
            jax.ShapeDtypeStruct((batch_n, SLOTS, width), F32),
            jax.ShapeDtypeStruct((2, SUB, LANES), F32),
        ),
        in_specs=[pl.BlockSpec(memory_space=pltpu.HBM)],
        out_specs=(whole, whole, whole, whole),
        scratch_shapes=[
            pltpu.VMEM((batch_n, TOTAL + 1, blocks, LANES), F32),
            pltpu.VMEM((batch_n, ROWS_KEPT, pieces, LANES), F32),
            pltpu.VMEM((height, LANES), F32),
            pltpu.VMEM((height, LANES), F32),
            pltpu.VMEM((batch_n, blocks, LANES), F32),
            pltpu.VMEM((batch_n, pieces, LANES), F32),
            pltpu.VMEM((batch_n, 3, blocks, LANES), F32),
            pltpu.VMEM((batch_n, 3, pieces, LANES), F32),
            pltpu.VMEM((2, batch_n, 2, row_n, pieces // 2, LANES), F32),
            pltpu.VMEM((2, batch_n, row_n, LANES), F32),
            pltpu.VMEM((2, batch_n, 1, col_n, blocks, LANES), F32),
            pltpu.VMEM((2, batch_n, col_n, LANES), F32),
            pltpu.SemaphoreType.DMA((batch_n, 2)),
            pltpu.SemaphoreType.DMA((batch_n,)),
            pltpu.SemaphoreType.DMA((batch_n, 3)),
            pltpu.SemaphoreType.DMA((2, batch_n, 3)),
            pltpu.SemaphoreType.DMA((batch_n, 2)),
            pltpu.SemaphoreType.DMA((2, batch_n, 2)),
            pltpu.SemaphoreType.DMA((col_n,)),
            pltpu.SemaphoreType.DMA,
            pltpu.SemaphoreType.DMA((col_n,)),
            pltpu.SemaphoreType.DMA,
            pltpu.SemaphoreType.DMA((batch_n,)),
            pltpu.SemaphoreType.DMA((batch_n, TOTAL)),
        ],
        compiler_params=pltpu.CompilerParams(
            collective_id=0, has_side_effects=True, vmem_limit_bytes=24 * 1024 * 1024
        ),
    )(w)


def update_kernel(mats, vx, yu, bid, out, diagonal, superdiag, left, right, stage, sems):
    batch_n, height, width = mats.shape
    pieces = width // LANES
    blocks = height // LANES
    row_place = lax.axis_index("row")
    col_place = lax.axis_index("col")
    slots = stage.shape[0]
    diagonal[...] = bid[0, 0:batch_n, 0:TOTAL]
    superdiag[...] = bid[1, 0:batch_n, 0:TOTAL]
    empty = jnp.zeros((LANES - 4 * SLOTS, LANES), F32)

    def halves(value):
        high = value.astype(jnp.bfloat16).astype(F32)
        return high, value - high

    def put_left(m, b):
        span = pl.ds(pl.multiple_of(b * LANES, LANES), LANES)
        high, low = halves(vx[m, :, span])
        stack = jnp.concatenate([high, high, low, low, empty], axis=0)
        left[lax.rem(b, 2)] = stack.T.astype(jnp.bfloat16)

    def put_right(m):
        for q in range(pieces):
            high, low = halves(yu[m, :, q * LANES : (q + 1) * LANES])
            stack = jnp.concatenate([high, low, high, low, empty], axis=0)
            right[:, q * LANES : (q + 1) * LANES] = stack.astype(jnp.bfloat16)

    def copies(at):
        slot = lax.rem(at, slots)
        m = at // blocks
        span = pl.ds(pl.multiple_of(lax.rem(at, blocks) * LANES, LANES), LANES)
        return [
            pltpu.make_async_copy(
                stage.at[slot, :, q * LANES : (q + 1) * LANES],
                out.at[m, span, q, :],
                sems.at[slot],
            )
            for q in range(pieces)
        ]

    def drain(at):
        slot = lax.rem(at, slots)
        pltpu.make_async_copy(stage.at[slot], stage.at[slot], sems.at[slot]).wait()

    lane_at = lax.broadcasted_iota(jnp.int32, (LANES, LANES), 1)

    def block_body(m, block):
        at = m * blocks + block
        slot = lax.rem(at, slots)
        span = pl.ds(pl.multiple_of(block * LANES, LANES), LANES)

        @pl.when(at >= slots)
        def _():
            drain(at)

        for q in range(0, pieces, 2):
            cut = slice(q * LANES, (q + 2) * LANES)
            change = jnp.dot(
                left[lax.rem(block, 2)], right[:, cut], preferred_element_type=F32
            )
            stage[slot, :, cut] = mats[m, span, cut] - change

        put_left(m, lax.rem(block + 1, blocks))

        @pl.when(col_place == 0)
        def _():
            stage[slot, :, 0:LANES] = jnp.where(lane_at < TOTAL, 0.0, stage[slot, :, 0:LANES])

        @pl.when((row_place == 0) & (block == 0))
        def _():
            stage[slot, 0:ROWS_KEPT, :] = jnp.where(
                lax.broadcasted_iota(jnp.int32, (ROWS_KEPT, width), 0) < TOTAL,
                0.0,
                stage[slot, 0:ROWS_KEPT, :],
            )

        for copy in copies(at):
            copy.start()

    for m in range(batch_n):
        put_left(m, 0)
        put_right(m)
        pl.loop(0, blocks)(functools.partial(block_body, m))

    for at in range(batch_n * blocks - slots, batch_n * blocks):
        drain(at)


def update_all(mats, vx, yu, bid):
    batch_n, height, width = mats.shape
    pieces = width // LANES
    whole = pl.BlockSpec(memory_space=pltpu.VMEM)
    slots = min(4, batch_n * height // LANES)
    return pl.pallas_call(
        update_kernel,
        out_shape=(
            jax.ShapeDtypeStruct((batch_n, height, pieces, LANES), F32),
            jax.ShapeDtypeStruct((batch_n, TOTAL), F32),
            jax.ShapeDtypeStruct((batch_n, TOTAL), F32),
        ),
        in_specs=[whole, whole, whole, whole],
        out_specs=(pl.BlockSpec(memory_space=pltpu.HBM), whole, whole),
        scratch_shapes=[
            pltpu.VMEM((2, LANES, LANES), jnp.bfloat16),
            pltpu.VMEM((LANES, width), jnp.bfloat16),
            pltpu.VMEM((slots, LANES, width), F32),
            pltpu.SemaphoreType.DMA((slots,)),
        ],
        compiler_params=pltpu.CompilerParams(vmem_limit_bytes=24 * 1024 * 1024),
    )(mats, vx, yu, bid)


def per_device(weights):
    batch_n, row_cycles, tile_len, col_cycles, _ = weights.shape
    height = row_cycles * tile_len
    parts = tile_len // LANES
    row_n = lax.axis_size("row")
    col_n = lax.axis_size("col")
    w = weights.reshape(batch_n, row_cycles, tile_len, col_cycles, parts, LANES)
    w = w.transpose(0, 1, 2, 4, 3, 5).reshape(batch_n, height, parts * col_cycles, LANES)
    mats, vx, yu, bid = factor_all(w, row_n, col_n, tile_len)
    out, diagonal, superdiag = update_all(mats, vx, yu, bid)
    out = out.reshape(batch_n, row_cycles, tile_len, parts, col_cycles, LANES)
    trailing = out.transpose(0, 1, 2, 4, 3, 5).reshape(weights.shape)
    return (trailing, diagonal, superdiag)


def solution(mesh):
    placed = (P(None, None, "row", None, "col"),)
    return jax.shard_map(
        per_device,
        mesh=mesh,
        in_specs=placed,
        out_specs=(P(None, None, "row", None, "col"), P(), P()),
        check_vma=False,
    )
```

```python
import functools

import jax
import jax.numpy as jnp
from jax import lax
from jax.experimental import pallas as pl
from jax.experimental.pallas import tpu as pltpu
from jax.sharding import PartitionSpec as P

STEPS = 6
PANELS = 2
TOTAL = STEPS * PANELS
SLOTS = 2 * TOTAL
LANES = 128
SUB = 8
ROWS_KEPT = 16
MESH = pl.DeviceIdType.MESH
F32 = jnp.float32


def reflect(leading, squares):
    length = jnp.sqrt(squares)
    divisor = jnp.maximum(leading + length, 1.0)
    factor = (leading + length) / jnp.maximum(length, 1.0)
    return (divisor, factor, -length)


def partner(me, d, count):
    if count & (count - 1):
        return lax.rem(me + d, count), lax.rem(me - d + count, count)
    to = me
    bit = 1
    while bit < count:
        if d & bit:
            to = to + bit - 2 * bit * lax.rem(me // bit, 2)
        bit *= 2
    return to, to


def peers(axis, count):
    me = lax.axis_index(axis)
    return [partner(me, d, count) for d in range(count - 1, 0, -1)]


def row_ids(blocks, tile_len, devices, place):
    at = lax.broadcasted_iota(jnp.int32, (blocks, LANES), 0) * LANES
    at = at + lax.broadcasted_iota(jnp.int32, (blocks, LANES), 1)
    return at // tile_len * (devices * tile_len) + place * tile_len + at % tile_len


def col_ids(pieces, tile_len, devices, place):
    cycles = pieces * LANES // tile_len
    q = lax.broadcasted_iota(jnp.int32, (pieces, LANES), 0)
    lane = lax.broadcasted_iota(jnp.int32, (pieces, LANES), 1)
    return q % cycles * (devices * tile_len) + place * tile_len + q // cycles * LANES + lane


def tree(parts):
    while len(parts) > 1:
        parts = [
            parts[i] + parts[i + 1] if i + 1 < len(parts) else parts[i]
            for i in range(0, len(parts), 2)
        ]
    return parts[0]


def put_row(ref, m, at, dense, first=0):
    span = pl.ds(pl.multiple_of(at // SUB * SUB, SUB), SUB)
    here = lax.broadcasted_iota(jnp.int32, (SUB, LANES), 0) == lax.rem(at, SUB)
    for q in range(dense.shape[0]):
        cut = slice((first + q) * LANES, (first + q + 1) * LANES)
        ref[m, span, cut] = jnp.where(here, dense[q : q + 1], ref[m, span, cut])


def small_row(dots, picks, squares, leading):
    at = lax.broadcasted_iota(jnp.int32, (SUB, LANES), 0)
    extra = jnp.where(at == 0, squares, jnp.where(at == 1, leading, 0.0))
    rest = jnp.zeros((LANES - 2 * SLOTS - SUB, LANES), F32)
    tile = jnp.concatenate([dots, picks, extra, rest], axis=0)
    return jnp.sum(tile.T, axis=0, keepdims=True)


def kernel(
    row_n, col_n, tile_len, w, mats, vx, yu, bid,
    cols, rows, spread, sums, cd, rd, base_c, base_r, row_big, row_small, col_big, col_small,
    load_sem, rows_sem, row_send, row_recv, col_send, col_recv,
    first_send, first_recv, cols_send, cols_recv, rows_send, rows_recv,
):
    batch_n, height, pieces, _ = w.shape
    blocks = height // LANES
    row_place = lax.axis_index("row")
    col_place = lax.axis_index("col")
    row_peers = peers("row", row_n)
    col_peers = peers("col", col_n)

    def load(m, q):
        return pltpu.make_async_copy(
            w.at[m, :, q, :], mats.at[m, :, q * LANES : (q + 1) * LANES], load_sem.at[m, min(q, 1)]
        )

    def load_rows(m):
        return pltpu.make_async_copy(w.at[m, pl.ds(0, ROWS_KEPT)], rows.at[m], rows_sem.at[m])

    for m in range(batch_n):
        load(m, 0).start()
    col_big[...] = jnp.zeros_like(col_big)
    col_small[...] = jnp.zeros_like(col_small)
    barrier = pltpu.get_barrier_semaphore()
    for axis, others in (("row", row_peers), ("col", col_peers)):
        for to, _ in others:
            pl.semaphore_signal(barrier, inc=1, device_id={axis: to}, device_id_type=MESH)

    @pl.when(row_place == 0)
    def _():
        for m in range(batch_n):
            load_rows(m).start()

    for m in range(batch_n):
        for q in range(1, pieces):
            load(m, q).start()

    vx[...] = jnp.zeros_like(vx)
    yu[...] = jnp.zeros_like(yu)
    bid[...] = jnp.zeros_like(bid)
    rd[...] = jnp.zeros_like(rd)
    pl.semaphore_wait(barrier, row_n + col_n - 2)

    def remote(ref, send, recv, axis, to):
        return pltpu.make_async_remote_copy(
            src_ref=ref,
            dst_ref=ref,
            send_sem=send,
            recv_sem=recv,
            device_id={axis: to},
            device_id_type=MESH,
        )

    def first_col(at, to):
        return remote(cols.at[:, 0], first_send.at[at], first_recv, "col", to)

    def later_cols(at, to):
        return remote(
            cols.at[:, pl.ds(1, TOTAL)], cols_send.at[at], cols_recv, "col", to
        )

    def row_copy(m, k, to):
        return remote(rows.at[m, k], rows_send.at[m], rows_recv.at[m, k], "row", to)

    def rows_sent(m):
        every = row_big.at[0, 0, pl.ds(0, 2), pl.ds(0, row_n - 1)]
        remote(every, rows_send.at[m], rows_recv.at[m, 0], "row", row_peers[0][0]).wait_send()

    for m in range(batch_n):
        load(m, 0).wait()

    @pl.when(col_place == 0)
    def _():
        for m in range(batch_n):
            for b in range(blocks):
                turned = mats[m, b * LANES : (b + 1) * LANES, 0:LANES].T
                cols[m, 0, b : b + 1, :] = turned[0:1]
                spread[(m * blocks + b) * SUB : (m * blocks + b + 1) * SUB, :] = turned[0:SUB]
                sums[(m * blocks + b) * SUB : (m * blocks + b + 1) * SUB, :] = turned[SUB : 2 * SUB]
        for at, (to, _) in enumerate(col_peers):
            first_col(at, to).start()
        for m in range(batch_n):
            for b in range(blocks):
                for j in range(1, TOTAL + 1):
                    held = spread if j < SUB else sums
                    at = (m * blocks + b) * SUB + j % SUB
                    cols[m, j, b : b + 1, :] = held[at : at + 1, :]
        for at, (to, _) in enumerate(col_peers):
            later_cols(at, to).start()

    @pl.when(row_place == 0)
    def _():
        for m in range(batch_n):
            load_rows(m).wait()
            for to, _ in row_peers:
                row_copy(m, 0, to).start()

    @pl.when(col_place != 0)
    def _():
        first_col(0, 0).wait_recv()

    grow = row_ids(blocks, tile_len, row_n, row_place)
    gcol = col_ids(pieces, tile_len, col_n, col_place)
    lane = lax.broadcasted_iota(jnp.int32, (1, LANES), 1)
    own_row = jnp.where(row_place == 0, lane, -1)
    own_col = jnp.where(col_place == 0, lane, -1)
    row_at = lax.broadcasted_iota(jnp.int32, (SUB, LANES), 0)
    lane_at = lax.broadcasted_iota(jnp.int32, (SUB, LANES), 1)

    half = pieces // 2

    def channel(axis, par, m, which):
        me = lax.axis_index(axis)
        small, big, sems, others = (
            (row_small, row_big, (row_send, row_recv), row_peers)
            if axis == "row"
            else (col_small, col_big, (col_send, col_recv), col_peers)
        )
        ref = small.at[par, m] if which == 0 else big.at[par, m, which - 1]
        own = ref.at[pl.ds(me, 1)]
        every = ref.at[pl.ds(0, len(others))]
        return own, every, (sems[0].at[m, which], sems[1].at[par, m, which]), others

    def post(axis, par, m, which):
        own, _, sems, others = channel(axis, par, m, which)
        for to, _ in others:
            remote(own, *sems, axis, to).start()

    def take(axis, par, m, which):
        _, every, sems, others = channel(axis, par, m, which)
        remote(every, *sems, axis, others[0][0]).wait_recv()

    def sent(axis, par, m, count):
        for which in range(count):
            _, every, sems, others = channel(axis, par, m, which)
            remote(every, *sems, axis, others[0][0]).wait_send()

    def sums_of(ref, par, m):
        total = jnp.sum(ref[par, m], axis=0, keepdims=True)
        turned = jnp.broadcast_to(total, (LANES, LANES)).T
        dots = turned[0:SLOTS]
        picks = turned[SLOTS : 2 * SLOTS]
        squares = turned[2 * SLOTS : 2 * SLOTS + 1]
        leading = turned[2 * SLOTS + 1 : 2 * SLOTS + 2]
        divisor, factor, bidiag = reflect(leading, squares)
        remain = 1.0 - leading / divisor
        weight = dots / divisor + picks * remain
        return divisor, factor, bidiag, remain, weight, picks

    def before_col(k, m):
        par = lax.rem(k + 1, 2)

        @pl.when(k > 0)
        def _():
            sent("row", par, m, 3)
            take("col", par, m, 0)

        divisor, factor, bidiag, remain, weight, picks = sums_of(col_small, par, m)
        bid[1] = jnp.where((row_at == m) & (lane_at == k - 1), bidiag, bid[1])
        row_vec = jnp.where(gcol == k, 1.0, rd[m] / divisor)
        row_vec = jnp.where(k > 0, row_vec, 0.0)
        at = jnp.where(k > 0, TOTAL - 1 + k, 0)
        put_row(yu, m, at, row_vec)
        column = cols[m, k]
        for b in range(blocks):
            old = vx[m, :, b * LANES : (b + 1) * LANES]
            base_c[m, 0, b : b + 1, :] = factor * (
                column[b : b + 1] * remain - jnp.sum(weight * old, axis=0, keepdims=True)
            )
            base_c[m, 1, b : b + 1, :] = column[b : b + 1] - jnp.sum(
                picks * old, axis=0, keepdims=True
            )
        base_c[m, 2] = jnp.broadcast_to(factor / divisor, (blocks, LANES))

    def new_col(k, m):
        par = lax.rem(k + 1, 2)

        @pl.when(k > 0)
        def _():
            take("col", par, m, 1)

        applied = tree([col_big[par, m, 0, s] for s in range(col_n)])
        image = jnp.where(grow >= k, base_c[m, 2] * applied + base_c[m, 0], 0.0)
        at = jnp.where(k > 0, TOTAL - 1 + k, 0)
        put_row(vx, m, at, image)
        return image

    def col_half(k, m):
        par = lax.rem(k, 2)
        image = new_col(k, m)
        piece = jnp.where(grow >= k, base_c[m, 1] - image, 0.0)
        cd[m] = piece

        def fill(b):
            spread[b * LANES : (b + 1) * LANES, :] = jnp.broadcast_to(
                cd[m, b : b + 1, :], (LANES, LANES)
            ).T

        fill(0)
        dots = tree(
            [
                vx[m, :, b * LANES : (b + 1) * LANES] * piece[b : b + 1]
                for b in range(blocks)
            ]
        )
        picks = jnp.where(own_row == k, vx[m, :, 0:LANES], 0.0)
        squares = jnp.sum(piece * piece, axis=0, keepdims=True)
        leading = jnp.sum(jnp.where(grow == k, piece, 0.0), axis=0, keepdims=True)
        small = small_row(dots, picks, squares, leading)
        for b in range(1, blocks):
            fill(b)
        for part in range(2):
            total = [None] * half
            for b in range(blocks):
                for g in range(LANES // SUB):
                    span = pl.ds(b * LANES + g * SUB, SUB)
                    by = spread[span, :]
                    for q in range(half):
                        at = (part * half + q) * LANES
                        term = mats[m, span, at : at + LANES] * by
                        total[q] = term if total[q] is None else total[q] + term
                if part == 0 and b == blocks // 2 - 1:
                    row_small[par, m, pl.ds(row_place, 1), :] = small
                    post("row", par, m, 0)
            for q in range(half):
                row_big[par, m, part, row_place, q : q + 1, :] = jnp.sum(
                    total[q], axis=0, keepdims=True
                )
            post("row", par, m, 1 + part)

    def before_row(k, m):
        par = lax.rem(k, 2)
        @pl.when(k > 0)
        def _():
            sent("col", par, m, 2)

        take("row", par, m, 0)

        @pl.when(row_place != 0)
        def _():
            row_copy(m, k, 0).wait_recv()

        divisor, factor, bidiag, remain, weight, picks = sums_of(row_small, par, m)
        bid[0] = jnp.where((row_at == m) & (lane_at == k), bidiag, bid[0])
        col_vec = jnp.where(grow == k, 1.0, cd[m] / divisor)
        put_row(vx, m, k, col_vec)
        row = rows[m, k]
        for q in range(pieces):
            old = yu[m, :, q * LANES : (q + 1) * LANES]
            base_r[m, 0, q : q + 1, :] = factor * (
                row[q : q + 1] * remain - jnp.sum(weight * old, axis=0, keepdims=True)
            )
            base_r[m, 1, q : q + 1, :] = row[q : q + 1] - jnp.sum(
                picks * old, axis=0, keepdims=True
            )
        base_r[m, 2] = jnp.broadcast_to(factor / divisor, (pieces, LANES))

    def row_half(k, m):
        par = lax.rem(k, 2)
        dots = squares = leading = None
        for part in range(2):
            tiles = slice(part * half, (part + 1) * half)
            take("row", par, m, 1 + part)
            trans = tree([row_big[par, m, part, s] for s in range(row_n)])
            here = gcol[tiles]
            image = jnp.where(here > k, base_r[m, 2, tiles] * trans + base_r[m, 0, tiles], 0.0)
            put_row(yu, m, k, image, part * half)
            piece = jnp.where(here > k, base_r[m, 1, tiles] - image, 0.0)
            rd[m, tiles] = piece
            terms = [
                yu[m, :, (part * half + q) * LANES : (part * half + q + 1) * LANES]
                * piece[q : q + 1]
                for q in range(half)
            ]
            dots = tree(terms if part == 0 else [dots] + terms)
            square = jnp.sum(piece * piece, axis=0, keepdims=True)
            lead = jnp.sum(jnp.where(here == k + 1, piece, 0.0), axis=0, keepdims=True)
            squares = square if part == 0 else squares + square
            leading = lead if part == 0 else leading + lead
            if part == 1:
                picks = jnp.where(own_col == k + 1, yu[m, :, 0:LANES], 0.0)
                small = small_row(dots, picks, squares, leading)
            scale = [
                jnp.broadcast_to(rd[m, part * half + q : part * half + q + 1, :], (SUB, LANES))
                for q in range(half)
            ]
            for b in range(blocks):
                groups = []
                for g in range(LANES // SUB):
                    span = pl.ds(b * LANES + g * SUB, SUB)
                    products = []
                    for q in range(half):
                        at = (part * half + q) * LANES
                        products.append(mats[m, span, at : at + LANES] * scale[q])
                    if part == 0:
                        sums[span, :] = tree(products)
                    else:
                        groups.append(tree(products) + sums[span, :])
                if part == 1:
                    turned = jnp.concatenate(groups, axis=0).T
                    col_big[par, m, 0, col_place, b : b + 1, :] = jnp.sum(
                        turned, axis=0, keepdims=True
                    )
                    if b == min(2, blocks - 1):
                        col_small[par, m, pl.ds(col_place, 1), :] = small
                        post("col", par, m, 0)
        post("col", par, m, 1)

    def step_body(k, carry):
        for m in range(batch_n):

            @pl.when(k == 0)
            def _():
                rest = mats.at[m, :, LANES:]
                pltpu.make_async_copy(rest, rest, load_sem.at[m, 1]).wait()

            before_col(k, m)
            col_half(k, m)

        @pl.when((row_place == 0) & (k < TOTAL - 1))
        def _():
            for m in range(batch_n):
                rows_sent(m)
                for to, _ in row_peers:
                    row_copy(m, k + 1, to).start()

        for m in range(batch_n):
            before_row(k, m)
            row_half(k, m)

        @pl.when((k == 0) & (col_place != 0))
        def _():
            later_cols(0, 0).wait_recv()

        return carry

    lax.fori_loop(0, TOTAL, step_body, 0)
    for m in range(batch_n):
        before_col(TOTAL, m)
        new_col(TOTAL, m)
        sent("col", (TOTAL + 1) % 2, m, 2)

    @pl.when(col_place == 0)
    def _():
        for at, (to, _) in enumerate(col_peers):
            first_col(at, to).wait_send()
            later_cols(at, to).wait_send()

    @pl.when(row_place == 0)
    def _():
        for m in range(batch_n):
            rows_sent(m)


def factor_all(w, row_n, col_n, tile_len):
    batch_n, height, pieces, _ = w.shape
    width = pieces * LANES
    blocks = height // LANES
    whole = pl.BlockSpec(memory_space=pltpu.VMEM)
    return pl.pallas_call(
        functools.partial(kernel, row_n, col_n, tile_len),
        out_shape=(
            jax.ShapeDtypeStruct((batch_n, height, width), F32),
            jax.ShapeDtypeStruct((batch_n, SLOTS, height), F32),
            jax.ShapeDtypeStruct((batch_n, SLOTS, width), F32),
            jax.ShapeDtypeStruct((2, SUB, LANES), F32),
        ),
        in_specs=[pl.BlockSpec(memory_space=pltpu.HBM)],
        out_specs=(whole, whole, whole, whole),
        scratch_shapes=[
            pltpu.VMEM((batch_n, TOTAL + 1, blocks, LANES), F32),
            pltpu.VMEM((batch_n, ROWS_KEPT, pieces, LANES), F32),
            pltpu.VMEM((height, LANES), F32),
            pltpu.VMEM((height, LANES), F32),
            pltpu.VMEM((batch_n, blocks, LANES), F32),
            pltpu.VMEM((batch_n, pieces, LANES), F32),
            pltpu.VMEM((batch_n, 3, blocks, LANES), F32),
            pltpu.VMEM((batch_n, 3, pieces, LANES), F32),
            pltpu.VMEM((2, batch_n, 2, row_n, pieces // 2, LANES), F32),
            pltpu.VMEM((2, batch_n, row_n, LANES), F32),
            pltpu.VMEM((2, batch_n, 1, col_n, blocks, LANES), F32),
            pltpu.VMEM((2, batch_n, col_n, LANES), F32),
            pltpu.SemaphoreType.DMA((batch_n, 2)),
            pltpu.SemaphoreType.DMA((batch_n,)),
            pltpu.SemaphoreType.DMA((batch_n, 3)),
            pltpu.SemaphoreType.DMA((2, batch_n, 3)),
            pltpu.SemaphoreType.DMA((batch_n, 2)),
            pltpu.SemaphoreType.DMA((2, batch_n, 2)),
            pltpu.SemaphoreType.DMA((col_n,)),
            pltpu.SemaphoreType.DMA,
            pltpu.SemaphoreType.DMA((col_n,)),
            pltpu.SemaphoreType.DMA,
            pltpu.SemaphoreType.DMA((batch_n,)),
            pltpu.SemaphoreType.DMA((batch_n, TOTAL)),
        ],
        compiler_params=pltpu.CompilerParams(
            collective_id=0, has_side_effects=True, vmem_limit_bytes=24 * 1024 * 1024
        ),
    )(w)


def update_kernel(
    mats, vx, yu, bid, out, diagonal, superdiag, left, right, stage, ends, sems, end_sems
):
    batch_n, height, width = mats.shape
    pieces = width // LANES
    blocks = height // LANES
    row_place = lax.axis_index("row")
    col_place = lax.axis_index("col")
    slots = stage.shape[0]
    finals = []
    for at, ref in enumerate((diagonal, superdiag)):
        ends[at] = bid[at, 0:batch_n, 0:TOTAL]
        finals.append(pltpu.make_async_copy(ends.at[at], ref, end_sems.at[at]))
    empty = jnp.zeros((LANES - 4 * SLOTS, LANES), F32)

    def halves(value):
        high = value.astype(jnp.bfloat16).astype(F32)
        return high, value - high

    def put_left(m, b):
        span = pl.ds(pl.multiple_of(b * LANES, LANES), LANES)
        high, low = halves(vx[m, :, span])
        stack = jnp.concatenate([high, high, low, low, empty], axis=0)
        left[lax.rem(b, 2)] = stack.T.astype(jnp.bfloat16)

    def put_right(m):
        for q in range(pieces):
            high, low = halves(yu[m, :, q * LANES : (q + 1) * LANES])
            stack = jnp.concatenate([high, low, high, low, empty], axis=0)
            right[:, q * LANES : (q + 1) * LANES] = stack.astype(jnp.bfloat16)

    def copies(at):
        slot = lax.rem(at, slots)
        m = at // blocks
        span = pl.ds(pl.multiple_of(lax.rem(at, blocks) * LANES, LANES), LANES)
        return [
            pltpu.make_async_copy(
                stage.at[slot, :, q * LANES : (q + 1) * LANES],
                out.at[m, span, q, :],
                sems.at[slot],
            )
            for q in range(pieces)
        ]

    def drain(at):
        slot = lax.rem(at, slots)
        pltpu.make_async_copy(stage.at[slot], stage.at[slot], sems.at[slot]).wait()

    lane_at = lax.broadcasted_iota(jnp.int32, (LANES, LANES), 1)

    def block_body(m, block):
        at = m * blocks + block
        slot = lax.rem(at, slots)
        span = pl.ds(pl.multiple_of(block * LANES, LANES), LANES)

        @pl.when(at >= slots)
        def _():
            drain(at)

        for q in range(0, pieces, 2):
            cut = slice(q * LANES, (q + 2) * LANES)
            change = jnp.dot(
                left[lax.rem(block, 2)], right[:, cut], preferred_element_type=F32
            )
            stage[slot, :, cut] = mats[m, span, cut] - change

        put_left(m, lax.rem(block + 1, blocks))

        @pl.when(col_place == 0)
        def _():
            stage[slot, :, 0:LANES] = jnp.where(lane_at < TOTAL, 0.0, stage[slot, :, 0:LANES])

        @pl.when((row_place == 0) & (block == 0))
        def _():
            stage[slot, 0:ROWS_KEPT, :] = jnp.where(
                lax.broadcasted_iota(jnp.int32, (ROWS_KEPT, width), 0) < TOTAL,
                0.0,
                stage[slot, 0:ROWS_KEPT, :],
            )

        for copy in copies(at):
            copy.start()

    for m in range(batch_n):
        put_left(m, 0)
        put_right(m)
        if m == 0:
            for copy in finals:
                copy.start()
        pl.loop(0, blocks)(functools.partial(block_body, m))

    for at in range(batch_n * blocks - slots, batch_n * blocks):
        drain(at)
    for copy in finals:
        copy.wait()


def update_all(mats, vx, yu, bid):
    batch_n, height, width = mats.shape
    pieces = width // LANES
    whole = pl.BlockSpec(memory_space=pltpu.VMEM)
    slots = min(4, batch_n * height // LANES)
    return pl.pallas_call(
        update_kernel,
        out_shape=(
            jax.ShapeDtypeStruct((batch_n, height, pieces, LANES), F32),
            jax.ShapeDtypeStruct((batch_n, TOTAL), F32),
            jax.ShapeDtypeStruct((batch_n, TOTAL), F32),
        ),
        in_specs=[whole, whole, whole, whole],
        out_specs=(pl.BlockSpec(memory_space=pltpu.HBM),) * 3,
        scratch_shapes=[
            pltpu.VMEM((2, LANES, LANES), jnp.bfloat16),
            pltpu.VMEM((LANES, width), jnp.bfloat16),
            pltpu.VMEM((slots, LANES, width), F32),
            pltpu.VMEM((2, batch_n, TOTAL), F32),
            pltpu.SemaphoreType.DMA((slots,)),
            pltpu.SemaphoreType.DMA((2,)),
        ],
        compiler_params=pltpu.CompilerParams(vmem_limit_bytes=24 * 1024 * 1024),
    )(mats, vx, yu, bid)


def per_device(weights):
    batch_n, row_cycles, tile_len, col_cycles, _ = weights.shape
    height = row_cycles * tile_len
    parts = tile_len // LANES
    row_n = lax.axis_size("row")
    col_n = lax.axis_size("col")
    w = weights.reshape(batch_n, row_cycles, tile_len, col_cycles, parts, LANES)
    w = w.transpose(0, 1, 2, 4, 3, 5).reshape(batch_n, height, parts * col_cycles, LANES)
    mats, vx, yu, bid = factor_all(w, row_n, col_n, tile_len)
    out, diagonal, superdiag = update_all(mats, vx, yu, bid)
    out = out.reshape(batch_n, row_cycles, tile_len, parts, col_cycles, LANES)
    trailing = out.transpose(0, 1, 2, 4, 3, 5).reshape(weights.shape)
    return (trailing, diagonal, superdiag)


def solution(mesh):
    placed = (P(None, None, "row", None, "col"),)
    return jax.shard_map(
        per_device,
        mesh=mesh,
        in_specs=placed,
        out_specs=(P(None, None, "row", None, "col"), P(), P()),
        check_vma=False,
    )
```
